32 devices in a mesh: dp: 8 (over z, core), mp: 4 (over y, x).
Axes of the slice: x: 2, y: 2, z: 4, core: 2. Of those that a mesh axis runs over, the one named last changes fastest.
Arguments:
- image_input: bfloat16 [16384, 1536], P(('dp', 'mp')), may hold values from -16 to 16
- text_input: bfloat16 [2560, 1536], P(('dp', 'mp')), may hold values from -16 to 16
- timesteps: int32 [16], replicated, may hold values from 0 to 999
- key_mask: int32 [16, 160], P('dp'), may hold values from 0 to 1, as said below
- mod_weight: bfloat16 [2, 2, 1536, 6, 1536], P(None, None, 'dp', None, 'mp'), may hold values from -0.21875 to 0.21875
- qkv_weight: bfloat16 [2, 2, 3, 1536, 1536], P(None, None, None, 'dp', 'mp'), may hold values from -0.15625 to 0.15625
- out_weight: bfloat16 [2, 2, 1536, 1536], P(None, None, 'mp', 'dp'), may hold values from -2.5 to 2.5
- up_weight: bfloat16 [2, 2, 1536, 6144], P(None, None, 'dp', 'mp'), may hold values from -0.15625 to 0.15625
- down_weight: bfloat16 [2, 2, 6144, 1536], P(None, None, 'mp', 'dp'), may hold values from -0.078125 to 0.078125
- image_cotangent: bfloat16 [16384, 1536], P(('dp', 'mp')), may hold values from -6 to 6
- text_cotangent: bfloat16 [2560, 1536], P(('dp', 'mp')), may hold values from -6 to 6
Outputs:
- image_output: bfloat16 [16384, 1536], P(('dp', 'mp'))
- text_output: bfloat16 [2560, 1536], P(('dp', 'mp'))
- image_grad: float32 [16384, 1536], P(('dp', 'mp'))
- text_grad: float32 [2560, 1536], P(('dp', 'mp'))
- grad_mod: float32 [2, 2, 1536, 6, 1536], P(None, None, 'dp', None, 'mp')
- grad_qkv: float32 [2, 2, 3, 1536, 1536], P(None, None, None, 'dp', 'mp')
- grad_out: float32 [2, 2, 1536, 1536], P(None, None, 'mp', 'dp')
- grad_up: float32 [2, 2, 1536, 6144], P(None, None, 'dp', 'mp')
- grad_down: float32 [2, 2, 6144, 1536], P(None, None, 'mp', 'dp')
The draws below stay inside these ranges and needn't reach their ends.
Inputs may be any that keep to these rules, and one draw needn't show every extreme that they name: `key_mask`: every row holds exactly 154 ones.
All inputs are finite; a program needn't handle non-finite values.
Results may differ from the reference program's by a relative error of at most 0.03.
Values may be sent and summed in bfloat16 or wider, within the bound.
A program may use at most 512 MiB of HBM per device.

```python
import math
import jax
import jax.numpy as jnp
from jax import lax

D = 1536
HEADS = 24
HEAD_DIM = 64
FF = 6144
IMG = 1024
TXT = 160
TXT_LIVE = 154
LAYERS = 2
SEQ_ALL = 16


def draw_stream(key, row_count):
    keys = jax.random.split(key, 3)
    base = jax.random.normal(keys[0], (row_count, D), jnp.float32)
    column_scale = jnp.exp(jax.random.uniform(keys[1], (1, D), jnp.float32, 0.0, math.log(10.0)))
    row_scale = jnp.exp(jax.random.uniform(keys[2], (row_count, 1), jnp.float32, math.log(0.5), math.log(2.0)))
    values = base * column_scale * row_scale * 0.22
    return jnp.clip(values, -16.0, 16.0).astype(jnp.bfloat16)


def draw_image_input(key, part):
    return draw_stream(jax.random.fold_in(key, 11), SEQ_ALL * IMG)


def draw_text_input(key, part):
    return draw_stream(jax.random.fold_in(key, 12), SEQ_ALL * TXT)


def shuffle_slots(row_key):
    return jax.random.permutation(row_key, TXT)


def draw_key_mask(key, part):
    row_keys = jax.random.split(jax.random.fold_in(key, 13), SEQ_ALL)
    order = jax.vmap(shuffle_slots)(row_keys)
    return (order < TXT_LIVE).astype(jnp.int32)


def set_ends(values, key, low, largest):
    shape = values.shape
    spot = [jax.random.randint(jax.random.fold_in(key, axis), (), 0, shape[axis]) for axis in range(len(shape))]
    values = values.at[tuple(spot)].set(low)
    longest = shape.index(max(shape))
    spot[longest] = (spot[longest] + 1) % shape[longest]
    return values.at[tuple(spot)].set(largest)


def spiked(drawn, key, source, target, shards_of, factor):
    def block_of(position):
        return (jnp.arange(drawn.shape[position]) // (drawn.shape[position] // shards_of)).reshape((-1,) + (1,) * (drawn.ndim - 1 - position))

    first = jax.random.permutation(key, shards_of)[block_of(target)]
    second = (block_of(target) + shards_of // 2) % shards_of
    return jnp.where((block_of(source) == first) | (block_of(source) == second), factor * drawn, drawn)


def block_levels(rng, dims, cuts, least, high):
    loudness, own = 1.0, jax.random.fold_in(rng, 6)
    for dim, blocks in cuts:
        draws = jnp.exp(jax.random.uniform(jax.random.fold_in(own, dim), (blocks,), jnp.float32, least / len(cuts), high / len(cuts)))
        loudness = loudness * jnp.repeat(draws, dims[dim] // blocks).reshape([-1 if axis == dim else 1 for axis in range(len(dims))])
    return loudness


def normal_values(rng, dims, scale, limit, cuts=(), kind=jnp.bfloat16):
    drawn = scale * jax.random.normal(rng, dims, jnp.float32)
    if cuts:
        drawn = drawn * block_levels(rng, dims, cuts, -0.22, 0.18)
    return jnp.clip(drawn, -limit, limit).astype(kind)


def noise_with(key, dims, deviation, limit, shards, heavy, held_as=jnp.bfloat16):
    values = deviation * jax.random.normal(key, dims, jnp.float32)
    if shards:
        values = values * block_levels(key, dims, shards, -0.22, 0.18)
    return jnp.clip(spiked(values, jax.random.fold_in(key, 3), *heavy), -limit, limit).astype(held_as)


def setup_inputs(seed: int = 0) -> dict:
    streams_of = jax.random.split(jax.random.key(seed), 12)
    image_input = draw_image_input(jax.random.fold_in(streams_of[11], 71), 0)
    text_input = draw_text_input(jax.random.fold_in(streams_of[11], 71), 0)
    timesteps = set_ends(jax.random.randint(streams_of[2], (SEQ_ALL,), 0, 1000), jax.random.fold_in(streams_of[2], 1), 0, 999).astype(jnp.int32)
    key_mask = draw_key_mask(jax.random.fold_in(streams_of[11], 71), 0)
    mod_weight = normal_values(streams_of[4], (LAYERS, 2, D, 6, D), (D // 2) ** -0.5, 0.21875, ((2, 8), (4, 4)))
    qkv_weight = normal_values(streams_of[5], (LAYERS, 2, 3, D, D), D ** -0.5, 0.15625, ((3, 8), (4, 4)))
    out_weight = normal_values(streams_of[6], (LAYERS, 2, D, D), (max(D // 256, 4)) ** -0.5, 2.5, ((2, 4), (3, 8)))
    up_weight = normal_values(streams_of[7], (LAYERS, 2, D, FF), D ** -0.5, 0.15625, ((2, 8), (3, 4)))
    down_weight = normal_values(streams_of[8], (LAYERS, 2, FF, D), FF ** -0.5, 0.078125, ((2, 4), (3, 8)))
    image_cotangent = noise_with(streams_of[9], (SEQ_ALL * IMG, D), 1.0, 6.0, ((0, 32),), (0, 1, 32, 2.75))
    text_cotangent = noise_with(streams_of[10], (SEQ_ALL * TXT, D), 1.0, 6.0, ((0, 32),), (0, 1, 32, 2.75))
    return dict(image_input=image_input, text_input=text_input, timesteps=timesteps, key_mask=key_mask, mod_weight=mod_weight, qkv_weight=qkv_weight, out_weight=out_weight, up_weight=up_weight, down_weight=down_weight, image_cotangent=image_cotangent, text_cotangent=text_cotangent)


@jax.custom_vjp
def low(v):
    return lax.optimization_barrier(v.astype(jnp.bfloat16)).astype(jnp.float32)

@jax.custom_vjp
def low_back(v):
    return v

def low_keep(v):
    return (low(v), None)

def low_pass(kept, grad):
    return (grad,)

def back_keep(v):
    return (v, None)

def back_low(kept, grad):
    return (low(grad),)
low.defvjp(low_keep, low_pass)
low_back.defvjp(back_keep, back_low)
HIGHEST = lax.Precision.HIGHEST
EPSILON = 1e-06

def conditioning(steps):
    half_width = D // 2
    frequency = jnp.exp(-math.log(10000.0) * jnp.arange(half_width, dtype=jnp.float32) / half_width)
    phases = steps.astype(jnp.float32)[..., None] * frequency
    embedded = jnp.concatenate([jnp.cos(phases), jnp.sin(phases)], axis=-1)
    return embedded / (1.0 + jnp.exp(-embedded))

def norm_mod(values, offset, stretch):
    centred = values - lax.optimization_barrier(jnp.mean(values, axis=-1, keepdims=True))
    variance = lax.optimization_barrier(jnp.mean(centred * centred, axis=-1, keepdims=True))
    return centred * lax.rsqrt(variance + EPSILON) * (1.0 + stretch) + offset

def gelu_tanh(values):
    return 0.5 * values * (1.0 + jnp.tanh(0.7978845608028654 * (values + 0.044715 * values * values * values)))

def one_sequence(weights, image_rows, text_rows, step, slot_mask):
    mod_weight, qkv_weight, out_weight, up_weight, down_weight = weights
    condition = low(conditioning(step))
    valid = jnp.concatenate([jnp.ones((IMG,), dtype=bool), slot_mask > 0])
    score_scale = HEAD_DIM ** (-0.5)
    streams = [image_rows, text_rows]
    for layer_index in range(LAYERS):
        modulation = [jnp.einsum('d,dkc->kc', condition, mod_weight[layer_index, stream], precision=HIGHEST) for stream in range(2)]
        normed = [low(norm_mod(streams[stream], modulation[stream][0], modulation[stream][1])) for stream in range(2)]
        projected = [low(low_back(jnp.einsum('nd,kdc->knc', normed[stream], qkv_weight[layer_index, stream], precision=HIGHEST))) for stream in range(2)]
        joined = jnp.concatenate(projected, axis=1).reshape(3, IMG + TXT, HEADS, HEAD_DIM)
        raw_scores = low_back(jnp.einsum('qhd,khd->hqk', joined[0], joined[1], precision=HIGHEST))
        scores = jnp.where(valid[None, None, :], raw_scores * score_scale, -1e+30)
        exponent = jnp.exp(scores - lax.optimization_barrier(jnp.max(scores, axis=-1, keepdims=True)))
        softmax_low = low(exponent / lax.optimization_barrier(jnp.sum(exponent, axis=-1, keepdims=True)))
        mixture = low(low_back(jnp.einsum('hqk,khd->qhd', softmax_low, joined[2], precision=HIGHEST))).reshape(IMG + TXT, D)
        pieces = [mixture[:IMG], mixture[IMG:]]
        updated = []
        for stream in range(2):
            gates = modulation[stream]
            branch_one = low_back(jnp.dot(pieces[stream], out_weight[layer_index, stream], precision=HIGHEST))
            middle = streams[stream] + gates[2] * branch_one
            hidden = low(norm_mod(middle, gates[3], gates[4]))
            pre_act = low_back(jnp.dot(hidden, up_weight[layer_index, stream], precision=HIGHEST))
            activation = low(gelu_tanh(pre_act))
            branch_two = low_back(jnp.dot(activation, down_weight[layer_index, stream], precision=HIGHEST))
            updated.append(middle + gates[5] * branch_two)
        streams = updated
    return (streams[0], streams[1])

def reference(image_input, text_input, timesteps, key_mask, mod_weight, qkv_weight, out_weight, up_weight, down_weight, image_cotangent, text_cotangent):
    weights = tuple((weight.astype(jnp.float32) for weight in (mod_weight, qkv_weight, out_weight, up_weight, down_weight)))
    image_rows = image_input.astype(jnp.float32).reshape(SEQ_ALL, IMG, D)
    text_rows = text_input.astype(jnp.float32).reshape(SEQ_ALL, TXT, D)

    def forward(weights, image_rows, text_rows):
        per_sequence = jax.checkpoint(one_sequence)

        def scan_step(carry, element):
            return (carry, per_sequence(weights, element[0], element[1], element[2], element[3]))
        unused, outputs = lax.scan(scan_step, jnp.zeros((), jnp.float32), (image_rows, text_rows, timesteps, key_mask))
        return outputs
    outputs, pullback = jax.vjp(forward, weights, image_rows, text_rows)
    image_back = image_cotangent.astype(jnp.float32).reshape(SEQ_ALL, IMG, D)
    text_back = text_cotangent.astype(jnp.float32).reshape(SEQ_ALL, TXT, D)
    weight_grads, image_grad, text_grad = pullback((image_back, text_back))
    return (outputs[0].reshape(SEQ_ALL * IMG, D).astype(jnp.bfloat16), outputs[1].reshape(SEQ_ALL * TXT, D).astype(jnp.bfloat16), image_grad.reshape(SEQ_ALL * IMG, D), text_grad.reshape(SEQ_ALL * TXT, D), weight_grads[0], weight_grads[1], weight_grads[2], weight_grads[3], weight_grads[4])
```

```python
import functools
import math

import jax
import jax.numpy as jnp
from jax import lax
from jax.experimental import pallas as pl
from jax.experimental.pallas import tpu as pltpu
from jax.sharding import PartitionSpec as P

HEAD_DIM = 64
LAYERS = 2
EPSILON = 1e-06
LOW = jnp.bfloat16
F32 = jnp.float32
PAIR=128
NT=(((1,),(1,)),((),()))
TN=(((0,),(0,)),((),()))
NN=(((1,),(0,)),((),()))
def dot(a,b,dims):
    return lax.dot_general(a,b,dims,preferred_element_type=jnp.float32)

def attn_fwd_kernel(scale,qb,mask_ref,qi,ki,vi,qt,kt,vt,oi,ot,li,lt):
    low = lax.broadcasted_iota(jnp.int32,(1,PAIR),1)<HEAD_DIM
    live = mask_ref[0:1,:]>0
    k_img,k_txt,v_img,v_txt=ki[...],kt[...],vi[...],vt[...]
    def block(q,store):
        q=q*jnp.asarray(scale,q.dtype)
        outs=[];lses=[]
        for h in range(2):
            keep = low if h==0 else jnp.logical_not(low)
            qm=jnp.where(keep,q,jnp.zeros_like(q))
            si=dot(qm,k_img,NT); st=jnp.where(live,dot(qm,k_txt,NT),-1e30)
            m=jnp.maximum(jnp.max(si,axis=-1,keepdims=True),jnp.max(st,axis=-1,keepdims=True))
            pi=jnp.exp(si-m); pt=jnp.exp(st-m)
            l=jnp.sum(pi,axis=-1,keepdims=True)+jnp.sum(pt,axis=-1,keepdims=True)
            o=dot(pi.astype(jnp.bfloat16),v_img,NN)+dot(pt.astype(jnp.bfloat16),v_txt,NN)
            outs.append(o/l); lses.append(m+jnp.log(l))
        store(jnp.where(low,outs[0],outs[1]).astype(jnp.bfloat16), jnp.where(low,lses[0],lses[1]))
    nb=qi.shape[0]//qb
    def body(b,c):
        r=pl.ds(pl.multiple_of(b*qb,qb),qb)
        def store(o,l):
            oi[r,:]=o; li[r,:]=l
        block(qi[r,:],store)
        return c
    lax.fori_loop(0,nb,body,0)
    def store(o,l):
        ot[...]=o; lt[...]=l
    block(qt[...],store)

def attn_fwd(img,txt,mask,qb=256):
    ri,c3=img.shape; rt=txt.shape[0]; c=c3//3; np_=c//PAIR
    spec=lambda r,off: pl.BlockSpec((r,PAIR),lambda j,off=off:(0,j+off*np_))
    f=pl.pallas_call(functools.partial(attn_fwd_kernel,HEAD_DIM**-0.5,qb),
        grid=(np_,),
        in_specs=[pl.BlockSpec((8,rt),lambda j:(0,0))]+[spec(ri,o) for o in range(3)]+[spec(rt,o) for o in range(3)],
        out_specs=[spec(ri,0),spec(rt,0),spec(ri,0),spec(rt,0)],
        out_shape=[jax.ShapeDtypeStruct((ri,c),jnp.bfloat16),jax.ShapeDtypeStruct((rt,c),jnp.bfloat16),
                   jax.ShapeDtypeStruct((ri,c),jnp.float32),jax.ShapeDtypeStruct((rt,c),jnp.float32)],
        compiler_params=pltpu.CompilerParams(vmem_limit_bytes=56<<20),
        cost_estimate=pl.CostEstimate(flops=4*(ri+rt)**2*c,bytes_accessed=(ri+rt)*c*12,transcendentals=(ri+rt)**2*c//HEAD_DIM),
        name="attn_fwd")
    return f(mask,img,img,img,txt,txt,txt)

def attn_bwd_kernel(scale,qb,mask_ref,qi,ki,vi,qt,kt,vt,oi,ot,li,lt,gi,gt,dqi,dki,dvi,dqt,dkt,dvt,aki,avi,akt,avt):
    low = lax.broadcasted_iota(jnp.int32,(1,PAIR),1)<HEAD_DIM
    live = mask_ref[:,0:1]>0
    k_img,k_txt,v_img,v_txt=ki[...],kt[...],vi[...],vt[...]
    for a in (aki,avi,akt,avt): a[...]=jnp.zeros_like(a)
    keeps=[low,jnp.logical_not(low)]
    kim=[jnp.where(k,k_img,jnp.zeros_like(k_img)) for k in keeps]
    ktm=[jnp.where(k,k_txt,jnp.zeros_like(k_txt)) for k in keeps]
    def block(q,o,l,g,store):
        q=q*jnp.asarray(scale,q.dtype)
        lT=l.T
        dT=(g.astype(jnp.float32)*o.astype(jnp.float32)).T
        dq=None
        for h in range(2):
            qm=jnp.where(keeps[h],q,jnp.zeros_like(q)); gm=jnp.where(keeps[h],g,jnp.zeros_like(g))
            lr=lT[h*HEAD_DIM:h*HEAD_DIM+1,:]
            dr=jnp.sum(dT[h*HEAD_DIM:(h+1)*HEAD_DIM,:],axis=0,keepdims=True)
            pi=jnp.exp(dot(k_img,qm,NT)-lr)
            pt=jnp.exp(jnp.where(live,dot(k_txt,qm,NT),-1e30)-lr)
            avi[...]+=dot(pi.astype(jnp.bfloat16),gm,NN)
            avt[...]+=dot(pt.astype(jnp.bfloat16),gm,NN)
            si=(pi*(dot(v_img,gm,NT)-dr)).astype(jnp.bfloat16)
            st=(pt*(dot(v_txt,gm,NT)-dr)).astype(jnp.bfloat16)
            aki[...]+=dot(si,qm,NN)
            akt[...]+=dot(st,qm,NN)
            d=dot(si,kim[h],TN)+dot(st,ktm[h],TN)
            dq=d if dq is None else dq+d
        store((dq*scale).astype(jnp.bfloat16))
    nb=qi.shape[0]//qb
    def body(b,c):
        r=pl.ds(pl.multiple_of(b*qb,qb),qb)
        def store(v): dqi[r,:]=v
        block(qi[r,:],oi[r,:],li[r,:],gi[r,:],store)
        return c
    lax.fori_loop(0,nb,body,0)
    def store(v): dqt[...]=v
    block(qt[...],ot[...],lt[...],gt[...],store)
    dki[...]=aki[...].astype(jnp.bfloat16); dvi[...]=avi[...].astype(jnp.bfloat16)
    dkt[...]=akt[...].astype(jnp.bfloat16); dvt[...]=avt[...].astype(jnp.bfloat16)

def attn_bwd(img,txt,mask,oi,ot,li,lt,gi,gt,qb=256):
    ri,c3=img.shape; rt=txt.shape[0]; c=c3//3; np_=c//PAIR
    spec=lambda r,off=0: pl.BlockSpec((r,PAIR),lambda j,off=off:(0,j+off*np_))
    f=pl.pallas_call(functools.partial(attn_bwd_kernel,HEAD_DIM**-0.5,qb),
        grid=(np_,),
        in_specs=[pl.BlockSpec((rt,128),lambda j:(0,0))]+[spec(ri,o) for o in range(3)]+[spec(rt,o) for o in range(3)]
            +[spec(ri),spec(rt)]*3,
        out_specs=[spec(ri)]*3+[spec(rt)]*3,
        out_shape=[jax.ShapeDtypeStruct((ri,c),jnp.bfloat16)]*3+[jax.ShapeDtypeStruct((rt,c),jnp.bfloat16)]*3,
        scratch_shapes=[pltpu.VMEM((ri,PAIR),jnp.float32)]*2+[pltpu.VMEM((rt,PAIR),jnp.float32)]*2,
        compiler_params=pltpu.CompilerParams(vmem_limit_bytes=56<<20),
        cost_estimate=pl.CostEstimate(flops=10*(ri+rt)**2*c,bytes_accessed=(ri+rt)*c*26,transcendentals=(ri+rt)**2*c//HEAD_DIM),
        name="attn_bwd")
    return f(mask,img,img,img,txt,txt,txt,oi,ot,li,lt,gi,gt)


def attention(img, txt, mask):
    c = img.shape[1] // 3
    pad = -c % PAIR
    if pad:
        img, txt = (jnp.pad(a.reshape(-1, 3, c), ((0, 0), (0, 0), (0, pad))).reshape(-1, 3 * (c + pad)) for a in (img, txt))
    mask_rows = jnp.broadcast_to(mask[None, :], (8, mask.shape[0]))
    oi, ot, li, lt = attn_fwd(img, txt, mask_rows, query_block(img.shape[0]))
    return (oi[:, :c], ot[:, :c]), (img, txt, oi, ot, li, lt)


def attention_back(kept, mask, grads):
    img, txt, oi, ot, li, lt = kept
    c = grads[0].shape[1]
    pad = oi.shape[1] - c
    gi, gt = (jnp.pad(g, ((0, 0), (0, pad))) for g in grads) if pad else grads
    mask_columns = jnp.broadcast_to(mask[:, None], (mask.shape[0], 128))
    out = attn_bwd(img, txt, mask_columns, oi, ot, li, lt, gi, gt, query_block(img.shape[0]))
    return tuple(jnp.concatenate([piece[:, :c] for piece in part], axis=1) for part in (out[:3], out[3:]))


def query_block(rows):
    return 256 if rows % 256 == 0 else rows


def conditioning(steps, width):
    half = width // 2
    frequency = jnp.exp(-math.log(10000.0) * jnp.arange(half, dtype=F32) / half)
    phases = steps.astype(F32)[..., None] * frequency
    embedded = jnp.concatenate([jnp.cos(phases), jnp.sin(phases)], axis=-1)
    return embedded / (1.0 + jnp.exp(-embedded))


def gelu(v):
    return 0.5 * v * (1.0 + jnp.tanh(0.7978845608028654 * (v + 0.044715 * v * v * v)))


def gelu_slope(v):
    inner = jnp.tanh(0.7978845608028654 * (v + 0.044715 * v * v * v))
    return 0.5 * (1.0 + inner) + 0.5 * v * (1.0 - inner * inner) * 0.7978845608028654 * (1.0 + 0.134145 * v * v)


def normed(v):
    centred = v - jnp.mean(v, axis=-1, keepdims=True)
    r = lax.rsqrt(jnp.mean(centred * centred, axis=-1, keepdims=True) + EPSILON)
    return centred * r, r


def norm_back(v, e):
    n, r = normed(v)
    return r * (e - jnp.mean(e, axis=-1, keepdims=True) - n * jnp.mean(e * n, axis=-1, keepdims=True)), n


def matmul(a, b, dims):
    return lax.dot_general(a, b, (dims, ((), ())), preferred_element_type=F32)


class Ring:
    def __init__(self, size):
        self.size = size
        half = size // 2
        self.order = list(range(half)) + list(range(size - 1, half - 1, -1))
        self.up = [(self.order[i], self.order[(i + 1) % size]) for i in range(size)]
        self.down = [(self.order[i], self.order[(i - 1) % size]) for i in range(size)]

    def offsets(self):
        out = [0]
        for t in range(1, self.size // 2):
            out += [-t, t]
        return out + [self.size // 2]

    def owners(self):
        place = {device: i for i, device in enumerate(self.order)}
        return [
            [self.order[(place[device] + offset) % self.size] for offset in self.offsets()]
            for device in range(self.size)
        ]

    def gather(self, x):
        cut = x.shape[0] // 16 * 8
        blocks, a, b = [x], x, x
        for _ in range(1, self.size // 2):
            a = lax.ppermute(a, "mp", self.up)
            b = lax.ppermute(b, "mp", self.down)
            blocks += [a, b]
        first = lax.ppermute(a[:cut], "mp", self.up)
        second = lax.ppermute(b[cut:], "mp", self.down)
        return blocks + [jnp.concatenate([first, second], axis=0)]

    def scatter(self, blocks):
        far = blocks[-1]
        cut = far.shape[0] // 16 * 8
        up = lax.ppermute(far[:cut], "mp", self.up)
        down = lax.ppermute(far[cut:], "mp", self.down)
        half = self.size // 2
        for t in range(half - 1, 0, -1):
            ahead, behind = blocks[2 * t], blocks[2 * t - 1]
            if t == half - 1:
                ahead = jnp.concatenate([add_low(ahead[:cut], up), ahead[cut:]], axis=0)
                behind = jnp.concatenate([behind[:cut], add_low(behind[cut:], down)], axis=0)
            else:
                ahead, behind = add_low(ahead, up), add_low(behind, down)
            up = lax.ppermute(ahead, "mp", self.up)
            down = lax.ppermute(behind, "mp", self.down)
        if half == 1:
            return blocks[0].astype(F32) + jnp.concatenate([up, down], axis=0).astype(F32)
        return blocks[0].astype(F32) + up.astype(F32) + down.astype(F32)


def add_low(a, b):
    return (a.astype(F32) + b.astype(F32)).astype(LOW)


class Step:
    def __init__(self, ring, image_rows, text_rows, keep):
        self.ring, self.image_rows, self.text_rows, self.keep = ring, image_rows, text_rows, keep

    def pick(self, modulation, member):
        return jnp.where(self.keep, modulation[0, member][None, :], modulation[1, member][None, :])

    def gather(self, x):
        blocks = self.ring.gather(x)
        r = self.image_rows
        return (
            jnp.concatenate([block[:r] for block in blocks], axis=0),
            jnp.concatenate([block[r:] for block in blocks], axis=0),
        )

    def scatter(self, parts):
        r, t = self.image_rows, self.text_rows
        return self.ring.scatter(
            [
                jnp.concatenate([parts[0][k * r : k * r + r], parts[1][k * t : k * t + t]], axis=0)
                for k in range(self.ring.size)
            ]
        )

    def forward(self, x, modulation, weights, mask):
        qkv, out, up, down = weights
        n1 = normed(x)[0] * (1.0 + self.pick(modulation, 1)) + self.pick(modulation, 0)
        rows1 = self.gather(n1.astype(LOW))
        proj = [matmul(rows1[s], qkv[s], ((1,), (0,))).astype(LOW) for s in range(2)]
        mixture, kept = attention(proj[0], proj[1], mask)
        branch1 = self.scatter([matmul(mixture[s], out[s], ((1,), (1,))).astype(LOW) for s in range(2)])
        middle = x + self.pick(modulation, 2) * branch1
        n2 = normed(middle)[0] * (1.0 + self.pick(modulation, 4)) + self.pick(modulation, 3)
        rows2 = self.gather(n2.astype(LOW))
        pre = [matmul(rows2[s], up[s], ((1,), (0,))) for s in range(2)]
        act = [gelu(pre[s]).astype(LOW) for s in range(2)]
        branch2 = self.scatter([matmul(act[s], down[s], ((1,), (1,))).astype(LOW) for s in range(2)])
        y = middle + self.pick(modulation, 5) * branch2
        return y, (x, modulation, rows1, kept, mixture, branch1, middle, rows2, pre, act, branch2)

    def sums(self, v):
        r = self.image_rows
        return jnp.stack([jnp.sum(v[:r], axis=0), jnp.sum(v[r:], axis=0)])

    def backward_mlp(self, g, saved, weights):
        qkv, out, up, down = weights
        x, modulation, rows1, kept, mixture, branch1, middle, rows2, pre, act, branch2 = saved
        db2 = self.gather((self.pick(modulation, 5) * g).astype(LOW))
        grad_act = [matmul(db2[s], down[s], ((1,), (0,))) for s in range(2)]
        d_pre = [(grad_act[s] * gelu_slope(pre[s])).astype(LOW) for s in range(2)]
        dn2 = self.scatter([matmul(d_pre[s], up[s], ((1,), (1,))).astype(LOW) for s in range(2)])
        inner, n = norm_back(middle, dn2 * (1.0 + self.pick(modulation, 4)))
        d_middle = g + inner
        mods = [self.sums(dn2), self.sums(dn2 * n), self.sums(g * branch2)]
        grads_down = [matmul(db2[s], act[s], ((0,), (0,))) for s in range(2)]
        grads_up = [matmul(rows2[s], d_pre[s], ((0,), (0,))) for s in range(2)]
        return d_middle, mods, grads_up, grads_down

    def backward_attention(self, d_middle, saved, weights, mask):
        qkv, out, up, down = weights
        x, modulation, rows1, kept, mixture, branch1, middle, rows2, pre, act, branch2 = saved
        db1 = self.gather((self.pick(modulation, 2) * d_middle).astype(LOW))
        d_mixture = [matmul(db1[s], out[s], ((1,), (0,))).astype(LOW) for s in range(2)]
        d_proj = attention_back(kept, mask, d_mixture)
        dn1 = self.scatter([matmul(d_proj[s], qkv[s], ((1,), (1,))).astype(LOW) for s in range(2)])
        inner, n = norm_back(x, dn1 * (1.0 + self.pick(modulation, 1)))
        mods = [self.sums(dn1), self.sums(dn1 * n), self.sums(d_middle * branch1)]
        grads_out = [matmul(db1[s], mixture[s], ((0,), (0,))) for s in range(2)]
        grads_qkv = [matmul(rows1[s], d_proj[s], ((0,), (0,))) for s in range(2)]
        return d_middle + inner, mods, grads_qkv, grads_out


def gather_weight(w):
    return lax.all_gather(w, "dp", axis=1, tiled=True)


def reduce_weight(parts):
    total = jnp.stack([sum(part[s] for part in parts).astype(LOW) for s in range(2)])
    return lax.psum_scatter(total, "dp", scatter_dimension=1, tiled=True).astype(F32)


def device_program(
    mp_size,
    image_input,
    text_input,
    timesteps,
    key_mask,
    mod_weight,
    qkv_weight,
    out_weight,
    up_weight,
    down_weight,
    image_cotangent,
    text_cotangent,
):
    seqs = key_mask.shape[0]
    assert seqs == 2
    width = image_input.shape[1]
    ring = Ring(mp_size)
    half = mp_size // 2
    side = lax.axis_index("mp") // half
    swap = [(i, (i + half) % mp_size) for i in range(mp_size)]
    ri, rt = image_input.shape[0] // 2, text_input.shape[0] // 2
    here = side == 0

    def deal(image, text):
        pieces = [jnp.concatenate([image[p * ri : p * ri + ri], text[p * rt : p * rt + rt]], axis=0) for p in range(2)]
        got = lax.ppermute(jnp.where(here, pieces[1], pieces[0]), "mp", swap)
        return [jnp.where(here, pieces[0], got).astype(F32), jnp.where(here, got, pieces[1]).astype(F32)]

    def undeal(rows):
        got = lax.ppermute(jnp.where(here, rows[1], rows[0]), "mp", swap)
        pieces = [jnp.where(here, rows[0], got), jnp.where(here, got, rows[1])]
        return (
            jnp.concatenate([piece[:ri] for piece in pieces], axis=0),
            jnp.concatenate([piece[ri:] for piece in pieces], axis=0),
        )

    condition = conditioning(timesteps, width).astype(LOW)
    depth = mod_weight.shape[2]
    own_condition = lax.dynamic_slice_in_dim(condition, lax.axis_index("dp") * depth, depth, axis=1)
    partial = jnp.einsum("nd,lsdkc->nlskc", own_condition, mod_weight, preferred_element_type=F32)
    own_mod = lax.psum_scatter(partial, "dp", scatter_dimension=0, tiled=True)
    modulation = lax.all_gather(own_mod, "mp", axis=4, tiled=True)

    owners = jnp.array(ring.owners(), dtype=jnp.int32)[lax.axis_index("mp")]
    segments = (owners % half) * 2 + owners // half
    masks = jnp.take(key_mask.reshape(seqs, mp_size, rt), segments, axis=1).reshape(seqs, -1)

    weights = []
    for l in range(LAYERS):
        weights.append(
            (
                gather_weight(jnp.swapaxes(qkv_weight[l], 1, 2).reshape(2, qkv_weight.shape[3], -1)),
                gather_weight(jnp.swapaxes(out_weight[l], 1, 2)),
                gather_weight(up_weight[l]),
                gather_weight(jnp.swapaxes(down_weight[l], 1, 2)),
            )
        )

    keep = (jnp.arange(ri + rt) < ri)[:, None]
    step = Step(ring, ri, rt, keep)
    rows = deal(image_input, text_input)
    upstream = deal(image_cotangent, text_cotangent)
    saved = []
    for l in range(LAYERS):
        done = [step.forward(rows[s], modulation[s, l], weights[l], masks[s]) for s in range(seqs)]
        rows = [d[0] for d in done]
        saved.append([d[1] for d in done])
    image_output, text_output = undeal([row.astype(LOW) for row in rows])

    reduced, mod_rows = [], []
    for l in reversed(range(LAYERS)):
        mlp = [step.backward_mlp(upstream[s], saved[l][s], weights[l]) for s in range(seqs)]
        grad_down = reduce_weight([m[3] for m in mlp])
        grad_up = reduce_weight([m[2] for m in mlp])
        att = [step.backward_attention(mlp[s][0], saved[l][s], weights[l], masks[s]) for s in range(seqs)]
        grad_out = reduce_weight([a[3] for a in att])
        grad_qkv = reduce_weight([a[2] for a in att])
        upstream = [a[0] for a in att]
        mod_rows.insert(0, jnp.stack([jnp.stack(att[s][1] + mlp[s][1], axis=1) for s in range(seqs)]))
        reduced.insert(0, (grad_qkv, grad_out, grad_up, grad_down))
    image_grad, text_grad = undeal(upstream)

    mod_sums = lax.psum_scatter(jnp.stack(mod_rows, axis=1), "mp", scatter_dimension=4, tiled=True)
    all_mods = lax.all_gather(mod_sums, "dp", axis=0, tiled=True)
    grad_mod = jnp.einsum("nd,nlskc->lsdkc", own_condition.astype(F32), all_mods, precision=lax.Precision.HIGHEST)
    columns = qkv_weight.shape[4]
    grad_qkv = jnp.stack(
        [jnp.swapaxes(r[0].reshape(2, -1, 3, columns), 1, 2) for r in reduced]
    )
    return (
        image_output,
        text_output,
        image_grad,
        text_grad,
        grad_mod,
        grad_qkv,
        jnp.stack([jnp.swapaxes(r[1], 1, 2) for r in reduced]),
        jnp.stack([r[2] for r in reduced]),
        jnp.stack([jnp.swapaxes(r[3], 1, 2) for r in reduced]),
    )


def solution(mesh):
    rows = P(("dp", "mp"), None)
    grads = (
        P(None, None, "dp", None, "mp"),
        P(None, None, None, "dp", "mp"),
        P(None, None, "mp", "dp"),
        P(None, None, "dp", "mp"),
        P(None, None, "mp", "dp"),
    )
    return jax.shard_map(
        functools.partial(device_program, mesh.shape["mp"]),
        mesh=mesh,
        in_specs=(rows, rows, P(), P("dp", None)) + grads + (rows, rows),
        out_specs=(rows, rows, rows, rows) + grads,
        check_vma=False,
    )
```

```python
import functools
import math

import jax
import jax.numpy as jnp
from jax import lax
from jax.experimental import pallas as pl
from jax.experimental.pallas import tpu as pltpu
from jax.sharding import PartitionSpec as P


HEAD_DIM = 64
LAYERS = 2
EPSILON = 1e-06
LOW = jnp.bfloat16
F32 = jnp.float32
PAIR=128
NT=(((1,),(1,)),((),()))
TN=(((0,),(0,)),((),()))
NN=(((1,),(0,)),((),()))


def dot(a,b,dims):
    return lax.dot_general(a,b,dims,preferred_element_type=jnp.float32)


def attn_fwd_kernel(scale,qb,mask_ref,qi,ki,vi,qt,kt,vt,oi,ot,li,lt):
    low = lax.broadcasted_iota(jnp.int32,(1,PAIR),1)<HEAD_DIM
    live = mask_ref[0:1,:]>0
    k_img,k_txt,v_img,v_txt=ki[...],kt[...],vi[...],vt[...]

    def block(q,store):
        q=q*jnp.asarray(scale,q.dtype)
        outs=[];lses=[]
        for h in range(2):
            keep = low if h==0 else jnp.logical_not(low)
            qm=jnp.where(keep,q,jnp.zeros_like(q))
            si=dot(qm,k_img,NT); st=jnp.where(live,dot(qm,k_txt,NT),-1e30)
            m=jnp.maximum(jnp.max(si,axis=-1,keepdims=True),jnp.max(st,axis=-1,keepdims=True))
            pi=jnp.exp(si-m); pt=jnp.exp(st-m)
            l=jnp.sum(pi,axis=-1,keepdims=True)+jnp.sum(pt,axis=-1,keepdims=True)
            o=dot(pi.astype(jnp.bfloat16),v_img,NN)+dot(pt.astype(jnp.bfloat16),v_txt,NN)
            outs.append(o/l); lses.append(m+jnp.log(l))
        store(jnp.where(low,outs[0],outs[1]).astype(jnp.bfloat16), jnp.where(low,lses[0],lses[1]))

    nb=qi.shape[0]//qb

    def body(b,c):
        r=pl.ds(pl.multiple_of(b*qb,qb),qb)

        def store(o,l):
            oi[r,:]=o; li[r,:]=l

        block(qi[r,:],store)
        return c

    lax.fori_loop(0,nb,body,0)

    def store(o,l):
        ot[...]=o; lt[...]=l

    block(qt[...],store)


def attn_fwd(img,txt,mask,qb=256):
    ri,c3=img.shape; rt=txt.shape[0]; c=c3//3; np_=c//PAIR
    spec=lambda r,off: pl.BlockSpec((r,PAIR),lambda j,off=off:(0,j+off*np_))
    f=pl.pallas_call(functools.partial(attn_fwd_kernel,HEAD_DIM**-0.5,qb),
        grid=(np_,),
        in_specs=[pl.BlockSpec((8,rt),lambda j:(0,0))]+[spec(ri,o) for o in range(3)]+[spec(rt,o) for o in range(3)],
        out_specs=[spec(ri,0),spec(rt,0),spec(ri,0),spec(rt,0)],
        out_shape=[jax.ShapeDtypeStruct((ri,c),jnp.bfloat16),jax.ShapeDtypeStruct((rt,c),jnp.bfloat16),
                   jax.ShapeDtypeStruct((ri,c),jnp.float32),jax.ShapeDtypeStruct((rt,c),jnp.float32)],
        compiler_params=pltpu.CompilerParams(vmem_limit_bytes=56<<20),
        cost_estimate=pl.CostEstimate(flops=4*(ri+rt)**2*c,bytes_accessed=(ri+rt)*c*12,transcendentals=(ri+rt)**2*c//HEAD_DIM),
        name="attn_fwd")
    return f(mask,img,img,img,txt,txt,txt)


def attn_bwd_kernel(scale,qb,mask_ref,qi,ki,vi,qt,kt,vt,oi,ot,li,lt,gi,gt,dqi,dki,dvi,dqt,dkt,dvt,aki,avi,akt,avt):
    low = lax.broadcasted_iota(jnp.int32,(1,PAIR),1)<HEAD_DIM
    live = mask_ref[:,0:1]>0
    k_img,k_txt,v_img,v_txt=ki[...],kt[...],vi[...],vt[...]
    for a in (aki,avi,akt,avt): a[...]=jnp.zeros_like(a)
    keeps=[low,jnp.logical_not(low)]
    kim=[jnp.where(k,k_img,jnp.zeros_like(k_img)) for k in keeps]
    ktm=[jnp.where(k,k_txt,jnp.zeros_like(k_txt)) for k in keeps]

    def block(q,o,l,g,store):
        q=q*jnp.asarray(scale,q.dtype)
        lT=l.T
        dT=(g.astype(jnp.float32)*o.astype(jnp.float32)).T
        dq=None
        for h in range(2):
            qm=jnp.where(keeps[h],q,jnp.zeros_like(q)); gm=jnp.where(keeps[h],g,jnp.zeros_like(g))
            lr=lT[h*HEAD_DIM:h*HEAD_DIM+1,:]
            dr=jnp.sum(dT[h*HEAD_DIM:(h+1)*HEAD_DIM,:],axis=0,keepdims=True)
            pi=jnp.exp(dot(k_img,qm,NT)-lr)
            pt=jnp.exp(jnp.where(live,dot(k_txt,qm,NT),-1e30)-lr)
            avi[...]+=dot(pi.astype(jnp.bfloat16),gm,NN)
            avt[...]+=dot(pt.astype(jnp.bfloat16),gm,NN)
            si=(pi*(dot(v_img,gm,NT)-dr)).astype(jnp.bfloat16)
            st=(pt*(dot(v_txt,gm,NT)-dr)).astype(jnp.bfloat16)
            aki[...]+=dot(si,qm,NN)
            akt[...]+=dot(st,qm,NN)
            d=dot(si,kim[h],TN)+dot(st,ktm[h],TN)
            dq=d if dq is None else dq+d
        store((dq*scale).astype(jnp.bfloat16))

    nb=qi.shape[0]//qb

    def body(b,c):
        r=pl.ds(pl.multiple_of(b*qb,qb),qb)

        def store(v): dqi[r,:]=v

        block(qi[r,:],oi[r,:],li[r,:],gi[r,:],store)
        return c

    lax.fori_loop(0,nb,body,0)

    def store(v): dqt[...]=v

    block(qt[...],ot[...],lt[...],gt[...],store)
    dki[...]=aki[...].astype(jnp.bfloat16); dvi[...]=avi[...].astype(jnp.bfloat16)
    dkt[...]=akt[...].astype(jnp.bfloat16); dvt[...]=avt[...].astype(jnp.bfloat16)


def attn_bwd(img,txt,mask,oi,ot,li,lt,gi,gt,qb=256):
    ri,c3=img.shape; rt=txt.shape[0]; c=c3//3; np_=c//PAIR
    spec=lambda r,off=0: pl.BlockSpec((r,PAIR),lambda j,off=off:(0,j+off*np_))
    f=pl.pallas_call(functools.partial(attn_bwd_kernel,HEAD_DIM**-0.5,qb),
        grid=(np_,),
        in_specs=[pl.BlockSpec((rt,128),lambda j:(0,0))]+[spec(ri,o) for o in range(3)]+[spec(rt,o) for o in range(3)]
            +[spec(ri),spec(rt)]*3,
        out_specs=[spec(ri)]*3+[spec(rt)]*3,
        out_shape=[jax.ShapeDtypeStruct((ri,c),jnp.bfloat16)]*3+[jax.ShapeDtypeStruct((rt,c),jnp.bfloat16)]*3,
        scratch_shapes=[pltpu.VMEM((ri,PAIR),jnp.float32)]*2+[pltpu.VMEM((rt,PAIR),jnp.float32)]*2,
        compiler_params=pltpu.CompilerParams(vmem_limit_bytes=56<<20),
        cost_estimate=pl.CostEstimate(flops=10*(ri+rt)**2*c,bytes_accessed=(ri+rt)*c*26,transcendentals=(ri+rt)**2*c//HEAD_DIM),
        name="attn_bwd")
    return f(mask,img,img,img,txt,txt,txt,oi,ot,li,lt,gi,gt)


def attention(img, txt, mask):
    c = img.shape[1] // 3
    pad = -c % PAIR
    if pad:
        img, txt = (jnp.pad(a.reshape(-1, 3, c), ((0, 0), (0, 0), (0, pad))).reshape(-1, 3 * (c + pad)) for a in (img, txt))
    mask_rows = jnp.broadcast_to(mask[None, :], (8, mask.shape[0]))
    oi, ot, li, lt = attn_fwd(img, txt, mask_rows, query_block(img.shape[0]))
    return (oi[:, :c], ot[:, :c]), (img, txt, oi, ot, li, lt)


def attention_back(kept, mask, grads):
    img, txt, oi, ot, li, lt = kept
    c = grads[0].shape[1]
    pad = oi.shape[1] - c
    gi, gt = (jnp.pad(g, ((0, 0), (0, pad))) for g in grads) if pad else grads
    mask_columns = jnp.broadcast_to(mask[:, None], (mask.shape[0], 128))
    out = attn_bwd(img, txt, mask_columns, oi, ot, li, lt, gi, gt, query_block(img.shape[0]))
    return tuple(jnp.concatenate([piece[:, :c] for piece in part], axis=1) for part in (out[:3], out[3:]))


def query_block(rows):
    return 256 if rows % 256 == 0 else rows


def conditioning(steps, width):
    half = width // 2
    frequency = jnp.exp(-math.log(10000.0) * jnp.arange(half, dtype=F32) / half)
    phases = steps.astype(F32)[..., None] * frequency
    embedded = jnp.concatenate([jnp.cos(phases), jnp.sin(phases)], axis=-1)
    return embedded / (1.0 + jnp.exp(-embedded))


def gelu(v):
    return 0.5 * v * (1.0 + jnp.tanh(0.7978845608028654 * (v + 0.044715 * v * v * v)))


def gelu_slope(v):
    inner = jnp.tanh(0.7978845608028654 * (v + 0.044715 * v * v * v))
    return 0.5 * (1.0 + inner) + 0.5 * v * (1.0 - inner * inner) * 0.7978845608028654 * (1.0 + 0.134145 * v * v)


def normed(v):
    centred = v - jnp.mean(v, axis=-1, keepdims=True)
    r = lax.rsqrt(jnp.mean(centred * centred, axis=-1, keepdims=True) + EPSILON)
    return centred * r, r


def matmul(a, b, dims):
    return lax.dot_general(a, b, (dims, ((), ())), preferred_element_type=F32)


class Ring:
    def __init__(self, size):
        self.size = size
        half = size // 2
        self.order = list(range(half)) + list(range(size - 1, half - 1, -1))
        self.up = [(self.order[i], self.order[(i + 1) % size]) for i in range(size)]
        self.down = [(self.order[i], self.order[(i - 1) % size]) for i in range(size)]

    def offsets(self):
        out = [0]
        for t in range(1, self.size // 2):
            out += [-t, t]
        return out + [self.size // 2]

    def owners(self):
        place = {device: i for i, device in enumerate(self.order)}
        return [
            [self.order[(place[device] + offset) % self.size] for offset in self.offsets()]
            for device in range(self.size)
        ]

    def shift(self, up, down):
        return lax.ppermute(up, "mp", self.up), lax.ppermute(down, "mp", self.down)

    def gather(self, x):
        cut = cut_of(x.shape[0])
        blocks, a, b = [x], x, x
        for _ in range(1, self.size // 2):
            a, b = self.shift(a, b)
            blocks += [a, b]
        first, second = self.shift(a[:cut], b[cut:])
        return blocks, (first, second)

    def scatter(self, image, text):
        rows, extra = image.shape[0] // self.size, text.shape[0] // self.size
        cut = cut_of(rows + extra)
        far = (self.size - 1) * rows
        second = jnp.concatenate([image[far + cut :], text[(self.size - 1) * extra :]], axis=0)
        up, down = self.shift(image[far : far + cut], second)
        half = self.size // 2
        if half == 1:
            full = jnp.concatenate([up, down], axis=0)
            return full, jnp.zeros_like(full)
        for t in range(half - 1, 0, -1):
            ahead, behind = ring_add(image, text, up, down, 2 * t, 2 * t - 1, rows, extra, t == half - 1)
            up, down = self.shift(ahead, behind)
        return up, down


def cut_of(rows):
    return rows // 32 * 16


def ring_add_kernel(halves, ia, ib, text, up, down, ahead, behind, ka, kb):
    rows, cut = ia.shape[0], up.shape[0]
    extra = ahead.shape[0] - rows
    wide = lambda v: v.astype(F32)
    ta = text[ka * extra : (ka + 1) * extra, :]
    tb = text[kb * extra : (kb + 1) * extra, :]
    if halves:
        ahead[:cut, :] = (wide(ia[:cut, :]) + wide(up[...])).astype(LOW)
        ahead[cut:rows, :] = ia[cut:, :]
        ahead[rows:, :] = ta
        behind[:cut, :] = ib[:cut, :]
        behind[cut:rows, :] = (wide(ib[cut:, :]) + wide(down[: rows - cut, :])).astype(LOW)
        behind[rows:, :] = (wide(tb) + wide(down[rows - cut :, :])).astype(LOW)
    else:
        for out, image, words, got in ((ahead, ia, ta, up), (behind, ib, tb, down)):
            out[:rows, :] = (wide(image[...]) + wide(got[:rows, :])).astype(LOW)
            out[rows:, :] = (wide(words) + wide(got[rows:, :])).astype(LOW)


def whole(a):
    return pl.BlockSpec(a.shape, lambda i: (0,) * len(a.shape))


def ring_add(image, text, up, down, ka, kb, rows, extra, halves):
    width = image.shape[1]
    out = jax.ShapeDtypeStruct((rows + extra, width), LOW)
    return pl.pallas_call(
        lambda *refs: ring_add_kernel(halves, *refs, ka, kb),
        grid=(1,),
        in_specs=[
            pl.BlockSpec((rows, width), lambda i: (ka, 0)),
            pl.BlockSpec((rows, width), lambda i: (kb, 0)),
            whole(text),
            whole(up),
            whole(down),
        ],
        out_specs=[whole(out)] * 2,
        out_shape=[out] * 2,
        cost_estimate=pl.CostEstimate(flops=rows * width, bytes_accessed=rows * width * 10, transcendentals=0),
        name="ring_add",
    )(image, image, text, up, down)


def row_loop(rows, extra, body):
    for stream, start, count in ((0, 0, rows), (1, rows, extra)):
        chunk = 16 if count % 16 == 0 else 8 if count % 8 == 0 else count
        if chunk == count:
            body(stream, pl.ds(start, count), pl.ds(0, count))
            continue

        def one(i, carry, stream=stream, start=start, chunk=chunk):
            off = pl.multiple_of(i * chunk, chunk)
            body(stream, pl.ds(pl.multiple_of(start + off, 8), chunk), pl.ds(off, chunk))
            return carry

        lax.fori_loop(0, count // chunk, one, 0)


def mean(v):
    return jnp.mean(v, axis=-1, keepdims=True)


def settle_kernel(rows, gate, norm, x, own, text, up, down, gates, norms, branch, y, n):
    def body(s, r, q):
        mine = own if s == 0 else text
        b = mine[q, :].astype(F32) + up[r, :].astype(F32) + down[r, :].astype(F32)
        branch[r, :] = b.astype(LOW)
        v = x[r, :] + gates[s, gate : gate + 1, :] * b
        y[r, :] = v.astype(y.dtype)
        if norm is not None:
            centred = v - mean(v)
            unit = centred * lax.rsqrt(mean(centred * centred) + EPSILON)
            n[r, :] = (unit * (1.0 + norms[s, norm + 1 : norm + 2, :]) + norms[s, norm : norm + 1, :]).astype(LOW)

    row_loop(rows, x.shape[0] - rows, body)


def settle(rows, gate, norm, x, image, text, up, down, gates, norms):
    height, width = x.shape
    shape = lambda kind: jax.ShapeDtypeStruct((height, width), kind)
    outs = [shape(LOW), shape(LOW if norm is None else F32)] + ([] if norm is None else [shape(LOW)])
    kernel = functools.partial(settle_kernel, rows, gate, norm)
    if norm is None:
        kernel = lambda *refs: settle_kernel(rows, gate, None, *refs, None)
    return pl.pallas_call(
        kernel,
        grid=(1,),
        in_specs=[whole(x), pl.BlockSpec((rows, width), lambda i: (0, 0))]
        + [whole(a) for a in (text, up, down, gates, norms)],
        out_specs=[whole(o) for o in outs],
        out_shape=outs,
        compiler_params=pltpu.CompilerParams(vmem_limit_bytes=40 << 20),
        cost_estimate=pl.CostEstimate(flops=20 * height * width, bytes_accessed=18 * height * width, transcendentals=0),
        name="settle",
    )(x, image, text, up, down, gates, norms)


def unsettle_kernel(rows, norm, gate, x, g, branch, own, text, up, down, norms, gates, d, low_out, sums):
    sums[...] = jnp.zeros_like(sums)

    def body(s, r, q):
        mine = own if s == 0 else text
        dn = mine[q, :].astype(F32) + up[r, :].astype(F32) + down[r, :].astype(F32)
        v, upstream = x[r, :], g[r, :]
        centred = v - mean(v)
        inverse = lax.rsqrt(mean(centred * centred) + EPSILON)
        n = centred * inverse
        e = dn * (1.0 + norms[s, norm + 1 : norm + 2, :])
        total = upstream + inverse * (e - mean(e) - n * mean(e * n))
        d[r, :] = total
        if gate is not None:
            low_out[r, :] = (gates[s, gate : gate + 1, :] * total).astype(LOW)
        for k, term in enumerate((dn, dn * n, upstream * branch[r, :].astype(F32))):
            sums[s * 3 + k : s * 3 + k + 1, :] += jnp.sum(term, axis=0, keepdims=True)

    row_loop(rows, x.shape[0] - rows, body)


def unsettle(rows, norm, gate, x, g, branch, image, text, up, down, norms, gates):
    height, width = x.shape
    outs = [jax.ShapeDtypeStruct((height, width), F32)]
    if gate is not None:
        outs.append(jax.ShapeDtypeStruct((height, width), LOW))
    outs.append(jax.ShapeDtypeStruct((8, width), F32))
    kernel = functools.partial(unsettle_kernel, rows, norm, gate)
    if gate is None:
        kernel = lambda *refs: unsettle_kernel(rows, norm, None, *refs[:-1], None, refs[-1])
    got = pl.pallas_call(
        kernel,
        grid=(1,),
        in_specs=[whole(x), whole(g), whole(branch), pl.BlockSpec((rows, width), lambda i: (0, 0))]
        + [whole(a) for a in (text, up, down, norms, gates)],
        out_specs=[whole(o) for o in outs],
        out_shape=outs,
        compiler_params=pltpu.CompilerParams(vmem_limit_bytes=40 << 20),
        cost_estimate=pl.CostEstimate(flops=40 * height * width, bytes_accessed=24 * height * width, transcendentals=0),
        name="unsettle",
    )(x, g, branch, image, text, up, down, norms, gates)
    sums = got[-1][:6].reshape(2, 3, width)
    return got[0], (got[1] if gate is not None else None), sums


class Step:
    def __init__(self, ring, image_rows, text_rows, keep):
        self.ring, self.image_rows, self.text_rows, self.keep = ring, image_rows, text_rows, keep

    def pick(self, modulation, member):
        return jnp.where(self.keep, modulation[0, member][None, :], modulation[1, member][None, :])

    def gather(self, x):
        blocks, (first, second) = self.ring.gather(x)
        r = self.image_rows
        rest = r - first.shape[0]
        return (
            jnp.concatenate([block[:r] for block in blocks] + [first, second[:rest]], axis=0),
            jnp.concatenate([block[r:] for block in blocks] + [second[rest:]], axis=0),
        )

    def product(self, a, b, dims):
        image = matmul(a[0], b[0], dims)
        return [image, matmul(a[1], b[1], dims)]

    def start(self, x, modulation):
        return normed(x)[0] * (1.0 + self.pick(modulation, 1)) + self.pick(modulation, 0)

    def forward(self, x, n1, modulation, following, weights, mask, held=None):
        qkv, out, up, down = weights
        rows1 = self.gather(n1)
        proj = low(self.product(rows1, qkv, ((1,), (0,))))
        mixture, kept = attention(proj[0], proj[1], mask)
        partial = low(self.product(mixture, out, ((1,), (1,))))
        got = self.ring.scatter(*partial)
        branch1, middle, n2 = settle(self.image_rows, 2, 3, x, *partial, *got, modulation, modulation)
        rows2 = self.gather(n2)
        if held is not None:
            image, held = tie(rows2[0], held)
            rows2 = (image, rows2[1])
        pre = self.product(rows2, up, ((1,), (0,)))
        act = low([gelu(p) for p in pre])
        partial = low(self.product(act, down, ((1,), (1,))))
        got = self.ring.scatter(*partial)
        if following is None:
            branch2, y = settle(self.image_rows, 5, None, middle, *partial, *got, modulation, modulation)
            n = None
        else:
            branch2, y, n = settle(self.image_rows, 5, 0, middle, *partial, *got, modulation, following)
        return y, n, (x, modulation, rows1, kept, mixture, branch1, middle, rows2, pre, act, branch2), held

    def backward_mlp(self, g, db2, saved, weights):
        _, _, up, down = weights
        _, modulation, _, _, _, _, middle, rows2, pre, act, branch2 = saved
        db2 = self.gather(db2)
        grad_act = self.product(db2, down, ((1,), (0,)))
        d_pre = low([grad_act[s] * gelu_slope(pre[s]) for s in range(2)])
        partial = low(self.product(d_pre, up, ((1,), (1,))))
        got = self.ring.scatter(*partial)
        d_middle, db1, mods = unsettle(
            self.image_rows, 3, 2, middle, g, branch2, *partial, *got, modulation, modulation
        )
        db1 = self.gather(db1)
        return d_middle, mods, db1, (rows2, d_pre), (db2, act)

    def backward_attention(self, d_middle, db1, saved, below, weights, mask):
        qkv, out, _, _ = weights
        x, modulation, rows1, kept, mixture, branch1, _, _, _, _, _ = saved
        d_mixture = low(self.product(db1, out, ((1,), (0,))))
        d_proj = attention_back(kept, mask, d_mixture)
        partial = low(self.product(d_proj, qkv, ((1,), (1,))))
        got = self.ring.scatter(*partial)
        g, db2, mods = unsettle(
            self.image_rows,
            0,
            None if below is None else 5,
            x,
            d_middle,
            branch1,
            *partial,
            *got,
            modulation,
            modulation if below is None else below,
        )
        return g, db2, mods, (rows1, d_proj), (db1, mixture)


def low(values):
    return [v.astype(LOW) for v in values]


def tie(*values):
    return lax.optimization_barrier(values)


def gather_weight(w):
    return lax.all_gather(w, "dp", axis=1, tiled=True)


def weight_grads(pairs):
    out = []
    for s in range(2):
        out.append(sum(matmul(a[s], b[s], ((0,), (0,))) for a, b in pairs).astype(LOW))
    return jnp.stack(out)


def reduce_weight(total):
    return lax.psum_scatter(total, "dp", scatter_dimension=1, tiled=True)


def exchange_sum(parts, axis):
    return jnp.sum(lax.all_to_all(parts, axis, split_axis=0, concat_axis=0, tiled=True), axis=0)


def device_program(
    mp_size,
    image_input,
    text_input,
    timesteps,
    key_mask,
    mod_weight,
    qkv_weight,
    out_weight,
    up_weight,
    down_weight,
    image_cotangent,
    text_cotangent,
):
    seqs = key_mask.shape[0]
    assert seqs == 2
    width = image_input.shape[1]
    ring = Ring(mp_size)
    half = mp_size // 2
    side = lax.axis_index("mp") // half
    swap = [(i, (i + half) % mp_size) for i in range(mp_size)]
    ri, rt = image_input.shape[0] // 2, text_input.shape[0] // 2
    here = side == 0

    def deal(image, text):
        pieces = [jnp.concatenate([image[p * ri : p * ri + ri], text[p * rt : p * rt + rt]], axis=0) for p in range(2)]
        got = lax.ppermute(jnp.where(here, pieces[1], pieces[0]), "mp", swap)
        return [jnp.where(here, pieces[0], got).astype(F32), jnp.where(here, got, pieces[1]).astype(F32)]

    def undeal(rows):
        got = lax.ppermute(jnp.where(here, rows[1], rows[0]), "mp", swap)
        pieces = [jnp.where(here, rows[0], got), jnp.where(here, got, rows[1])]
        return (
            jnp.concatenate([piece[:ri] for piece in pieces], axis=0),
            jnp.concatenate([piece[ri:] for piece in pieces], axis=0),
        )

    condition = conditioning(timesteps, width).astype(LOW)
    depth = mod_weight.shape[2]
    own_condition = lax.dynamic_slice_in_dim(condition, lax.axis_index("dp") * depth, depth, axis=1)
    partial = jnp.einsum("nd,lsdkc->nlskc", own_condition, mod_weight, preferred_element_type=F32)
    columns = mod_weight.shape[4]
    own_mod = exchange_sum(partial.reshape(-1, seqs * LAYERS * 12, columns), "dp")
    modulation = lax.all_gather(own_mod, "mp", axis=0)
    modulation = jnp.swapaxes(modulation, 0, 1).reshape(seqs, LAYERS, 2, 6, width)

    owners = jnp.array(ring.owners(), dtype=jnp.int32)[lax.axis_index("mp")]
    segments = (owners % half) * 2 + owners // half
    masks = jnp.take(key_mask.reshape(seqs, mp_size, rt), segments, axis=1).reshape(seqs, -1)

    weights = []
    for l in range(LAYERS):
        weights.append(
            (
                gather_weight(jnp.swapaxes(qkv_weight[l], 1, 2).reshape(2, qkv_weight.shape[3], -1)),
                gather_weight(jnp.swapaxes(out_weight[l], 1, 2)),
                gather_weight(up_weight[l]),
                gather_weight(jnp.swapaxes(down_weight[l], 1, 2)),
            )
        )

    keep = (jnp.arange(ri + rt) < ri)[:, None]
    step = Step(ring, ri, rt, keep)
    rows = deal(image_input, text_input)
    upstream = deal(image_cotangent, text_cotangent)
    saved = []
    mods = [[modulation[s, l] for l in range(LAYERS)] + [None] for s in range(seqs)]
    ready = [low([step.start(rows[s], mods[s][0])])[0] for s in range(seqs)]
    last = LAYERS - 1
    db2 = [low([step.pick(mods[s][last], 5) * upstream[s]])[0] for s in range(seqs)]
    for l in range(LAYERS):
        done = [
            step.forward(rows[s], ready[s], mods[s][l], mods[s][l + 1], weights[l], masks[s], None if l else db2[s])
            for s in range(seqs)
        ]
        rows, ready = [d[0] for d in done], [d[1] for d in done]
        saved.append([d[2] for d in done])
        if l == 0:
            db2 = [d[3] for d in done]
    image_output, text_output = undeal(rows)

    reduced, mod_rows = [None] * LAYERS, [None] * LAYERS
    for l in reversed(range(LAYERS)):
        mlp = [step.backward_mlp(upstream[s], db2[s], saved[l][s], weights[l]) for s in range(seqs)]
        down_total = weight_grads([m[4] for m in mlp])
        up_total = weight_grads([m[3] for m in mlp])
        db1 = [m[2] for m in mlp]
        grad_down = reduce_weight(down_total)
        grad_up = reduce_weight(up_total)
        if l < last:
            (image, text), above_up, above_down = tie(db1[1], reduced[l + 1][2], reduced[l + 1][3])
            db1[1] = (image, text)
            reduced[l + 1][2:] = [above_up, above_down]
        att = [
            step.backward_attention(mlp[s][0], db1[s], saved[l][s], mods[s][l - 1] if l else None, weights[l], masks[s])
            for s in range(seqs)
        ]
        out_total = weight_grads([a[4] for a in att])
        qkv_total = weight_grads([a[3] for a in att])
        upstream, db2 = [a[0] for a in att], [a[1] for a in att]
        if l:
            db2[1], out_total, qkv_total = tie(db2[1], out_total, qkv_total)
        grad_out = reduce_weight(out_total)
        grad_qkv = reduce_weight(qkv_total)
        mod_rows[l] = jnp.stack([jnp.concatenate([att[s][2], mlp[s][1]], axis=1) for s in range(seqs)])
        reduced[l] = [grad_qkv, grad_out, grad_up, grad_down]
    image_grad, text_grad = undeal(upstream)
    reduced = [[r.astype(F32) for r in layer] for layer in reduced]

    mod_rows = jnp.stack(mod_rows, axis=1).reshape(-1, mp_size, columns)
    mod_sums = exchange_sum(jnp.swapaxes(mod_rows, 0, 1).reshape(mp_size, -1, columns), "mp")
    all_mods = lax.all_gather(mod_sums, "dp", axis=0).reshape(-1, LAYERS, 2, 6, columns)
    grad_mod = jnp.einsum("nd,nlskc->lsdkc", own_condition.astype(F32), all_mods, precision=lax.Precision.HIGHEST)
    grad_qkv = jnp.stack(
        [jnp.swapaxes(r[0].reshape(2, -1, 3, columns), 1, 2) for r in reduced]
    )
    return (
        image_output,
        text_output,
        image_grad,
        text_grad,
        grad_mod,
        grad_qkv,
        jnp.stack([jnp.swapaxes(r[1], 1, 2) for r in reduced]),
        jnp.stack([r[2] for r in reduced]),
        jnp.stack([jnp.swapaxes(r[3], 1, 2) for r in reduced]),
    )


def solution(mesh):
    rows = P(("dp", "mp"), None)
    grads = (
        P(None, None, "dp", None, "mp"),
        P(None, None, None, "dp", "mp"),
        P(None, None, "mp", "dp"),
        P(None, None, "dp", "mp"),
        P(None, None, "mp", "dp"),
    )

    def program(*arrays):
        return device_program(mesh.shape["mp"], *arrays)

    return jax.shard_map(
        program,
        mesh=mesh,
        in_specs=(rows, rows, P(), P("dp", None)) + grads + (rows, rows),
        out_specs=(rows, rows, rows, rows) + grads,
        check_vma=False,
    )
```

```python
import functools
import math

import jax
import jax.numpy as jnp
from jax import lax
from jax.experimental import pallas as pl
from jax.experimental.pallas import tpu as pltpu
from jax.sharding import PartitionSpec as P


HEAD_DIM = 64
LAYERS = 2
EPSILON = 1e-06
LOW = jnp.bfloat16
F32 = jnp.float32
PAIR=128
NT=(((1,),(1,)),((),()))
TN=(((0,),(0,)),((),()))
NN=(((1,),(0,)),((),()))


def dot(a,b,dims):
    return lax.dot_general(a,b,dims,preferred_element_type=jnp.float32)


def attn_fwd_kernel(scale,qb,mask_ref,qi,ki,vi,qt,kt,vt,oi,ot,li,lt):
    low = lax.broadcasted_iota(jnp.int32,(1,PAIR),1)<HEAD_DIM
    live = mask_ref[0:1,:]>0
    k_img,k_txt,v_img,v_txt=ki[...],kt[...],vi[...],vt[...]

    def block(q,store):
        q=q*jnp.asarray(scale,q.dtype)
        outs=[];lses=[]
        for h in range(2):
            keep = low if h==0 else jnp.logical_not(low)
            qm=jnp.where(keep,q,jnp.zeros_like(q))
            si=dot(qm,k_img,NT); st=jnp.where(live,dot(qm,k_txt,NT),-1e30)
            m=jnp.maximum(jnp.max(si,axis=-1,keepdims=True),jnp.max(st,axis=-1,keepdims=True))
            pi=jnp.exp(si-m); pt=jnp.exp(st-m)
            l=jnp.sum(pi,axis=-1,keepdims=True)+jnp.sum(pt,axis=-1,keepdims=True)
            o=dot(pi.astype(jnp.bfloat16),v_img,NN)+dot(pt.astype(jnp.bfloat16),v_txt,NN)
            outs.append(o/l); lses.append(m+jnp.log(l))
        store(jnp.where(low,outs[0],outs[1]).astype(jnp.bfloat16), jnp.where(low,lses[0],lses[1]))

    nb=qi.shape[0]//qb

    def body(b,c):
        r=pl.ds(pl.multiple_of(b*qb,qb),qb)

        def store(o,l):
            oi[r,:]=o; li[r,:]=l

        block(qi[r,:],store)
        return c

    lax.fori_loop(0,nb,body,0)

    def store(o,l):
        ot[...]=o; lt[...]=l

    block(qt[...],store)


def attn_fwd(img,txt,mask,qb=256):
    ri,c3=img.shape; rt=txt.shape[0]; c=c3//3; np_=c//PAIR
    spec=lambda r,off: pl.BlockSpec((r,PAIR),lambda j,off=off:(0,j+off*np_))
    f=pl.pallas_call(functools.partial(attn_fwd_kernel,HEAD_DIM**-0.5,qb),
        grid=(np_,),
        in_specs=[pl.BlockSpec((8,rt),lambda j:(0,0))]+[spec(ri,o) for o in range(3)]+[spec(rt,o) for o in range(3)],
        out_specs=[spec(ri,0),spec(rt,0),spec(ri,0),spec(rt,0)],
        out_shape=[jax.ShapeDtypeStruct((ri,c),jnp.bfloat16),jax.ShapeDtypeStruct((rt,c),jnp.bfloat16),
                   jax.ShapeDtypeStruct((ri,c),jnp.float32),jax.ShapeDtypeStruct((rt,c),jnp.float32)],
        compiler_params=pltpu.CompilerParams(vmem_limit_bytes=56<<20),
        cost_estimate=pl.CostEstimate(flops=4*(ri+rt)**2*c,bytes_accessed=(ri+rt)*c*12,transcendentals=(ri+rt)**2*c//HEAD_DIM),
        name="attn_fwd")
    return f(mask,img,img,img,txt,txt,txt)


def attn_bwd_kernel(scale,qb,mask_ref,qi,ki,vi,qt,kt,vt,oi,ot,li,lt,gi,gt,dqi,dki,dvi,dqt,dkt,dvt,aki,avi,akt,avt):
    low = lax.broadcasted_iota(jnp.int32,(1,PAIR),1)<HEAD_DIM
    live = mask_ref[:,0:1]>0
    k_img,k_txt,v_img,v_txt=ki[...],kt[...],vi[...],vt[...]
    for a in (aki,avi,akt,avt): a[...]=jnp.zeros_like(a)
    keeps=[low,jnp.logical_not(low)]
    kim=[jnp.where(k,k_img,jnp.zeros_like(k_img)) for k in keeps]
    ktm=[jnp.where(k,k_txt,jnp.zeros_like(k_txt)) for k in keeps]

    def block(q,o,l,g,store):
        q=q*jnp.asarray(scale,q.dtype)
        lT=l.T
        dT=(g.astype(jnp.float32)*o.astype(jnp.float32)).T
        dq=None
        for h in range(2):
            qm=jnp.where(keeps[h],q,jnp.zeros_like(q)); gm=jnp.where(keeps[h],g,jnp.zeros_like(g))
            lr=lT[h*HEAD_DIM:h*HEAD_DIM+1,:]
            dr=jnp.sum(dT[h*HEAD_DIM:(h+1)*HEAD_DIM,:],axis=0,keepdims=True)
            pi=jnp.exp(dot(k_img,qm,NT)-lr)
            pt=jnp.exp(jnp.where(live,dot(k_txt,qm,NT),-1e30)-lr)
            avi[...]+=dot(pi.astype(jnp.bfloat16),gm,NN)
            avt[...]+=dot(pt.astype(jnp.bfloat16),gm,NN)
            si=(pi*(dot(v_img,gm,NT)-dr)).astype(jnp.bfloat16)
            st=(pt*(dot(v_txt,gm,NT)-dr)).astype(jnp.bfloat16)
            aki[...]+=dot(si,qm,NN)
            akt[...]+=dot(st,qm,NN)
            d=dot(si,kim[h],TN)+dot(st,ktm[h],TN)
            dq=d if dq is None else dq+d
        store((dq*scale).astype(jnp.bfloat16))

    nb=qi.shape[0]//qb

    def body(b,c):
        r=pl.ds(pl.multiple_of(b*qb,qb),qb)

        def store(v): dqi[r,:]=v

        block(qi[r,:],oi[r,:],li[r,:],gi[r,:],store)
        return c

    lax.fori_loop(0,nb,body,0)

    def store(v): dqt[...]=v

    block(qt[...],ot[...],lt[...],gt[...],store)
    dki[...]=aki[...].astype(jnp.bfloat16); dvi[...]=avi[...].astype(jnp.bfloat16)
    dkt[...]=akt[...].astype(jnp.bfloat16); dvt[...]=avt[...].astype(jnp.bfloat16)


def attn_bwd(img,txt,mask,oi,ot,li,lt,gi,gt,qb=256):
    ri,c3=img.shape; rt=txt.shape[0]; c=c3//3; np_=c//PAIR
    spec=lambda r,off=0: pl.BlockSpec((r,PAIR),lambda j,off=off:(0,j+off*np_))
    f=pl.pallas_call(functools.partial(attn_bwd_kernel,HEAD_DIM**-0.5,qb),
        grid=(np_,),
        in_specs=[pl.BlockSpec((rt,128),lambda j:(0,0))]+[spec(ri,o) for o in range(3)]+[spec(rt,o) for o in range(3)]
            +[spec(ri),spec(rt)]*3,
        out_specs=[spec(ri)]*3+[spec(rt)]*3,
        out_shape=[jax.ShapeDtypeStruct((ri,c),jnp.bfloat16)]*3+[jax.ShapeDtypeStruct((rt,c),jnp.bfloat16)]*3,
        scratch_shapes=[pltpu.VMEM((ri,PAIR),jnp.float32)]*2+[pltpu.VMEM((rt,PAIR),jnp.float32)]*2,
        compiler_params=pltpu.CompilerParams(vmem_limit_bytes=56<<20),
        cost_estimate=pl.CostEstimate(flops=10*(ri+rt)**2*c,bytes_accessed=(ri+rt)*c*26,transcendentals=(ri+rt)**2*c//HEAD_DIM),
        name="attn_bwd")
    return f(mask,img,img,img,txt,txt,txt,oi,ot,li,lt,gi,gt)


def attention(img, txt, mask):
    c = img.shape[1] // 3
    pad = -c % PAIR
    if pad:
        img, txt = (jnp.pad(a.reshape(-1, 3, c), ((0, 0), (0, 0), (0, pad))).reshape(-1, 3 * (c + pad)) for a in (img, txt))
    mask_rows = jnp.broadcast_to(mask[None, :], (8, mask.shape[0]))
    oi, ot, li, lt = attn_fwd(img, txt, mask_rows, query_block(img.shape[0]))
    return (oi[:, :c], ot[:, :c]), (img, txt, oi, ot, li, lt)


def attention_back(kept, mask, grads):
    img, txt, oi, ot, li, lt = kept
    c = grads[0].shape[1]
    pad = oi.shape[1] - c
    gi, gt = (jnp.pad(g, ((0, 0), (0, pad))) for g in grads) if pad else grads
    mask_columns = jnp.broadcast_to(mask[:, None], (mask.shape[0], 128))
    out = attn_bwd(img, txt, mask_columns, oi, ot, li, lt, gi, gt, query_block(img.shape[0]))
    return tuple([piece[:, :c] for piece in part] for part in (out[:3], out[3:]))


def query_block(rows):
    return 256 if rows % 256 == 0 else rows


def conditioning(steps, width):
    half = width // 2
    frequency = jnp.exp(-math.log(10000.0) * jnp.arange(half, dtype=F32) / half)
    phases = steps.astype(F32)[..., None] * frequency
    embedded = jnp.concatenate([jnp.cos(phases), jnp.sin(phases)], axis=-1)
    return embedded / (1.0 + jnp.exp(-embedded))


def normed(v):
    centred = v - jnp.mean(v, axis=-1, keepdims=True)
    r = lax.rsqrt(jnp.mean(centred * centred, axis=-1, keepdims=True) + EPSILON)
    return centred * r, r


class Ring:
    def __init__(self, size):
        self.size = size
        half = size // 2
        self.order = list(range(half)) + list(range(size - 1, half - 1, -1))
        self.up = [(self.order[i], self.order[(i + 1) % size]) for i in range(size)]
        self.down = [(self.order[i], self.order[(i - 1) % size]) for i in range(size)]

    def offsets(self):
        out = [0]
        for t in range(1, self.size // 2):
            out += [-t, t]
        return out + [self.size // 2]

    def owners(self):
        place = {device: i for i, device in enumerate(self.order)}
        return [
            [self.order[(place[device] + offset) % self.size] for offset in self.offsets()]
            for device in range(self.size)
        ]

    def shift(self, up, down):
        return lax.ppermute(up, "mp", self.up), lax.ppermute(down, "mp", self.down)

    def gather(self, x):
        cut = cut_of(x.shape[0])
        blocks, a, b = [x], x, x
        for _ in range(1, self.size // 2):
            a, b = self.shift(a, b)
            blocks += [a, b]
        first, second = self.shift(a[:cut], b[cut:])
        return blocks, (first, second)

    def scatter(self, image, text, first, second):
        rows, extra = image.shape[0] // self.size, text.shape[0] // self.size
        up, down = self.shift(first, second)
        half = self.size // 2
        if half == 1:
            full = jnp.concatenate([up, down], axis=0)
            return full, jnp.zeros_like(full)
        for t in range(half - 1, 0, -1):
            ahead, behind = ring_add(image, text, up, down, 2 * t, 2 * t - 1, rows, extra, t == half - 1)
            up, down = self.shift(ahead, behind)
        return up, down


def cut_of(rows):
    return rows // 32 * 16


def ring_add_kernel(halves, ia, ib, text, up, down, ahead, behind, ka, kb):
    rows, cut = ia.shape[0], up.shape[0]
    extra = ahead.shape[0] - rows
    wide = lambda v: v.astype(F32)
    ta = text[ka * extra : (ka + 1) * extra, :]
    tb = text[kb * extra : (kb + 1) * extra, :]
    if halves:
        ahead[:cut, :] = (wide(ia[:cut, :]) + wide(up[...])).astype(LOW)
        ahead[cut:rows, :] = ia[cut:, :]
        ahead[rows:, :] = ta
        behind[:cut, :] = ib[:cut, :]
        behind[cut:rows, :] = (wide(ib[cut:, :]) + wide(down[: rows - cut, :])).astype(LOW)
        behind[rows:, :] = (wide(tb) + wide(down[rows - cut :, :])).astype(LOW)
    else:
        for out, image, words, got in ((ahead, ia, ta, up), (behind, ib, tb, down)):
            out[:rows, :] = (wide(image[...]) + wide(got[:rows, :])).astype(LOW)
            out[rows:, :] = (wide(words) + wide(got[rows:, :])).astype(LOW)


def whole(a):
    return pl.BlockSpec(a.shape, lambda i: (0,) * len(a.shape))


def ring_add(image, text, up, down, ka, kb, rows, extra, halves):
    width = image.shape[1]
    out = jax.ShapeDtypeStruct((rows + extra, width), LOW)
    return pl.pallas_call(
        lambda *refs: ring_add_kernel(halves, *refs, ka, kb),
        grid=(1,),
        in_specs=[
            pl.BlockSpec((rows, width), lambda i: (ka, 0)),
            pl.BlockSpec((rows, width), lambda i: (kb, 0)),
            whole(text),
            whole(up),
            whole(down),
        ],
        out_specs=[whole(out)] * 2,
        out_shape=[out] * 2,
        cost_estimate=pl.CostEstimate(flops=rows * width, bytes_accessed=rows * width * 10, transcendentals=0),
        name="ring_add",
    )(image, image, text, up, down)


def row_loop(rows, extra, body):
    for stream, start, count in ((0, 0, rows), (1, rows, extra)):
        chunk = 16 if count % 16 == 0 else 8 if count % 8 == 0 else count
        if chunk == count:
            body(stream, pl.ds(start, count), pl.ds(0, count))
            continue

        def one(i, carry, stream=stream, start=start, chunk=chunk):
            off = pl.multiple_of(i * chunk, chunk)
            body(stream, pl.ds(pl.multiple_of(start + off, 8), chunk), pl.ds(off, chunk))
            return carry

        lax.fori_loop(0, count // chunk, one, 0)


def mean(v):
    return jnp.mean(v, axis=-1, keepdims=True)


def settle_kernel(rows, gate, norm, x, own, text, up, down, gates, norms, branch, y, n):
    def body(s, r, q):
        mine = own if s == 0 else text
        b = mine[q, :].astype(F32) + up[r, :].astype(F32) + down[r, :].astype(F32)
        branch[r, :] = b.astype(LOW)
        v = x[r, :] + gates[s, gate : gate + 1, :] * b
        y[r, :] = v.astype(y.dtype)
        if norm is not None:
            centred = v - mean(v)
            unit = centred * lax.rsqrt(mean(centred * centred) + EPSILON)
            n[r, :] = (unit * (1.0 + norms[s, norm + 1 : norm + 2, :]) + norms[s, norm : norm + 1, :]).astype(LOW)

    row_loop(rows, x.shape[0] - rows, body)


def settle(rows, gate, norm, x, image, text, up, down, gates, norms):
    height, width = x.shape
    shape = lambda kind: jax.ShapeDtypeStruct((height, width), kind)
    outs = [shape(LOW), shape(LOW if norm is None else F32)] + ([] if norm is None else [shape(LOW)])
    kernel = functools.partial(settle_kernel, rows, gate, norm)
    if norm is None:
        kernel = lambda *refs: settle_kernel(rows, gate, None, *refs, None)
    return pl.pallas_call(
        kernel,
        grid=(1,),
        in_specs=[whole(x), pl.BlockSpec((rows, width), lambda i: (0, 0))]
        + [whole(a) for a in (text, up, down, gates, norms)],
        out_specs=[whole(o) for o in outs],
        out_shape=outs,
        compiler_params=pltpu.CompilerParams(vmem_limit_bytes=40 << 20),
        cost_estimate=pl.CostEstimate(flops=20 * height * width, bytes_accessed=18 * height * width, transcendentals=0),
        name="settle",
    )(x, image, text, up, down, gates, norms)


def unsettle_kernel(rows, norm, gate, x, g, branch, own, text, up, down, norms, gates, d, low_out, sums):
    sums[...] = jnp.zeros_like(sums)

    def body(s, r, q):
        mine = own if s == 0 else text
        dn = mine[q, :].astype(F32) + up[r, :].astype(F32) + down[r, :].astype(F32)
        v, upstream = x[r, :], g[r, :]
        centred = v - mean(v)
        inverse = lax.rsqrt(mean(centred * centred) + EPSILON)
        n = centred * inverse
        e = dn * (1.0 + norms[s, norm + 1 : norm + 2, :])
        total = upstream + inverse * (e - mean(e) - n * mean(e * n))
        d[r, :] = total
        if gate is not None:
            low_out[r, :] = (gates[s, gate : gate + 1, :] * total).astype(LOW)
        for k, term in enumerate((dn, dn * n, upstream * branch[r, :].astype(F32))):
            sums[s * 3 + k : s * 3 + k + 1, :] += jnp.sum(term, axis=0, keepdims=True)

    row_loop(rows, x.shape[0] - rows, body)


def unsettle(rows, norm, gate, x, g, branch, image, text, up, down, norms, gates):
    height, width = x.shape
    outs = [jax.ShapeDtypeStruct((height, width), F32)]
    if gate is not None:
        outs.append(jax.ShapeDtypeStruct((height, width), LOW))
    outs.append(jax.ShapeDtypeStruct((8, width), F32))
    kernel = functools.partial(unsettle_kernel, rows, norm, gate)
    if gate is None:
        kernel = lambda *refs: unsettle_kernel(rows, norm, None, *refs[:-1], None, refs[-1])
    got = pl.pallas_call(
        kernel,
        grid=(1,),
        in_specs=[whole(x), whole(g), whole(branch), pl.BlockSpec((rows, width), lambda i: (0, 0))]
        + [whole(a) for a in (text, up, down, norms, gates)],
        out_specs=[whole(o) for o in outs],
        out_shape=outs,
        compiler_params=pltpu.CompilerParams(vmem_limit_bytes=40 << 20),
        cost_estimate=pl.CostEstimate(flops=40 * height * width, bytes_accessed=24 * height * width, transcendentals=0),
        name="unsettle",
    )(x, g, branch, image, text, up, down, norms, gates)
    sums = got[-1][:6].reshape(2, 3, width)
    return got[0], (got[1] if gate is not None else None), sums


PARAMS = pltpu.CompilerParams(vmem_limit_bytes=58 << 20)


def tile_of(columns):
    return 384 if columns % 384 == 0 else columns


def halves_of(rows):
    step = rows // 2 if rows % 32 == 0 and rows > 512 else rows
    return [slice(i, i + step) for i in range(0, rows, step)]


def spread_kernel(mode, count, *refs):
    blocks, (first, second, wi, wt), rest = refs[:count], refs[count : count + 4], refs[count + 4 :]
    slopes, rest = (rest[:2], rest[2:]) if mode == "slope" else (None, rest)
    ri, rt, out = rest[0], rest[1], rest[2:]

    @pl.when(pl.program_id(0) == 0)
    def _():
        r, e, cut = ri.shape[0] // (count + 1), rt.shape[0] // (count + 1), first.shape[0]
        for k, block in enumerate(blocks):
            ri[k * r : (k + 1) * r, :] = block[:r, :]
            rt[k * e : (k + 1) * e, :] = block[r:, :]
        ri[count * r : count * r + cut, :] = first[...]
        ri[count * r + cut :, :] = second[: r - cut, :]
        rt[count * e :, :] = second[r - cut :, :]

    for s, (rows, w) in enumerate(((ri, wi), (rt, wt))):
        for part in halves_of(rows.shape[0]):
            v = dot(rows[part, :], w[...], NN)
            if mode == "gelu":
                t = jnp.tanh(0.7978845608028654 * (v + 0.044715 * v * v * v))
                half = 0.5 * (1.0 + t)
                out[s][part, :] = (v * half).astype(LOW)
                bend = 0.7978845608028654 * (1.0 + 0.134145 * v * v)
                out[2 + s][part, :] = (half + 0.5 * v * (1.0 - t * t) * bend).astype(LOW)
            elif mode == "slope":
                out[s][part, :] = (v * slopes[s][part, :].astype(F32)).astype(LOW)
            else:
                out[s][part, :] = v.astype(LOW)


def spread_product(mode, rows, pieces, weight, slopes=()):
    blocks, (first, second) = pieces
    count = len(blocks)
    size = count + 1
    height, depth = blocks[0].shape
    columns = weight.shape[2]
    tile = tile_of(columns)
    heights = (rows * size, (height - rows) * size)
    wide = [pl.BlockSpec((h, tile), lambda j: (0, j)) for h in heights]
    products = 4 if mode == "gelu" else 2
    return pl.pallas_call(
        functools.partial(spread_kernel, mode, count),
        grid=(columns // tile,),
        in_specs=[whole(a) for a in (*blocks, first, second)]
        + [pl.BlockSpec((None, depth, tile), lambda j, s=s: (s, 0, j)) for s in range(2)]
        + (wide if slopes else []),
        out_specs=[pl.BlockSpec((h, depth), lambda j: (0, 0)) for h in heights] + wide * (products // 2),
        out_shape=[jax.ShapeDtypeStruct((h, depth), LOW) for h in heights]
        + [jax.ShapeDtypeStruct((h, columns), LOW) for h in heights] * (products // 2),
        compiler_params=PARAMS,
        cost_estimate=pl.CostEstimate(
            flops=2 * sum(heights) * depth * columns,
            bytes_accessed=4 * depth * columns + 4 * sum(heights) * (depth + columns),
            transcendentals=0,
        ),
        name="spread",
    )(*blocks, first, second, weight, weight, *slopes)


def collect_kernel(count, size, *refs):
    xs = (refs[:count], refs[count : 2 * count])
    ws = (refs[2 * count : 3 * count], refs[3 * count : 4 * count])
    pi, pt, first, second = refs[4 * count :]
    for out, x, w in zip((pi, pt), *zip(*((xs[s], ws[s]) for s in range(2)))):
        for part in halves_of(out.shape[0]):
            out[part, :] = sum(dot(a[part, :], b[...], NT) for a, b in zip(x, w)).astype(LOW)
    r, e, cut = pi.shape[0] // size, pt.shape[0] // size, first.shape[0]
    far = (size - 1) * r
    first[...] = pi[far : far + cut, :]
    second[: r - cut, :] = pi[far + cut :, :]
    second[r - cut :, :] = pt[(size - 1) * e :, :]


def collect_product(size, image, text, weight):
    count, group = len(image), image[0].shape[1]
    height, extra = image[0].shape[0], text[0].shape[0]
    width = weight.shape[1]
    tile = tile_of(width)
    cut = cut_of((height + extra) // size)
    rest = (height + extra) // size - cut
    outs = (height, extra, cut, rest)
    return pl.pallas_call(
        functools.partial(collect_kernel, count, size),
        grid=(width // tile,),
        in_specs=[whole(a) for a in (*image, *text)]
        + [pl.BlockSpec((None, tile, group), lambda j, s=s, k=k: (s, j, k)) for s in range(2) for k in range(count)],
        out_specs=[pl.BlockSpec((h, tile), lambda j: (0, j)) for h in outs],
        out_shape=[jax.ShapeDtypeStruct((h, width), LOW) for h in outs],
        compiler_params=PARAMS,
        cost_estimate=pl.CostEstimate(
            flops=2 * (height + extra) * width * group * count,
            bytes_accessed=4 * width * group * count + 2 * (height + extra) * (width + group * count),
            transcendentals=0,
        ),
        name="collect",
    )(*image, *text, *([weight] * (2 * count)))


def grad_kernel(seqs, count, *refs):
    out = refs[-1]
    per = 2 * (1 + count)
    for s in range(2):
        for k in range(count):
            total = None
            for q in range(seqs):
                mine = refs[q * per + s * (1 + count) : q * per + (s + 1) * (1 + count)]
                v = dot(mine[0][...], mine[1 + k][...], TN)
                total = v if total is None else total + v
            columns = total.shape[1]
            out[s, :, k * columns : (k + 1) * columns] = total.astype(LOW)


def grad_product(pairs):
    seqs, count = len(pairs), len(pairs[0][0][1])
    width = pairs[0][0][0].shape[1]
    columns = count * pairs[0][0][1][0].shape[1]
    tile = 256 if width % 256 == 0 else width
    arrays, specs, rows = [], [], 0
    for pair in pairs:
        for a, bs in pair:
            arrays += [a, *bs]
            specs += [pl.BlockSpec((a.shape[0], tile), lambda i: (0, i))] + [whole(b) for b in bs]
            rows += a.shape[0]
    return pl.pallas_call(
        functools.partial(grad_kernel, seqs, count),
        grid=(width // tile,),
        in_specs=specs,
        out_specs=pl.BlockSpec((2, tile, columns), lambda i: (0, i, 0)),
        out_shape=jax.ShapeDtypeStruct((2, width, columns), LOW),
        compiler_params=PARAMS,
        cost_estimate=pl.CostEstimate(
            flops=2 * rows * width * columns,
            bytes_accessed=4 * width * columns + 2 * rows * (width + columns),
            transcendentals=0,
        ),
        name="grad",
    )(*arrays)


class Step:
    def __init__(self, ring, image_rows, text_rows, keep):
        self.ring, self.image_rows, self.text_rows, self.keep = ring, image_rows, text_rows, keep

    def pick(self, modulation, member):
        return jnp.where(self.keep, modulation[0, member][None, :], modulation[1, member][None, :])

    def spread(self, mode, pieces, weight, slopes=()):
        got = spread_product(mode, self.image_rows, pieces, weight, slopes)
        return got[:2], got[2:]

    def collect(self, image, text, weight):
        if image[0].shape[1] % 128:
            image, text = ([jnp.concatenate(a, axis=1)] for a in (image, text))
        return collect_product(self.ring.size, image, text, weight)

    def start(self, x, modulation):
        return normed(x)[0] * (1.0 + self.pick(modulation, 1)) + self.pick(modulation, 0)

    def forward(self, x, n1, modulation, following, weights, mask, held=None):
        qkv, out, up, down = weights
        pieces = self.ring.gather(n1)
        rows1, proj = self.spread("", pieces, qkv)
        mixture, kept = attention(proj[0], proj[1], mask)
        partial = self.collect(mixture[:1], mixture[1:], out)
        got = self.ring.scatter(*partial)
        branch1, middle, n2 = settle(self.image_rows, 2, 3, x, *partial[:2], *got, modulation, modulation)
        pieces = self.ring.gather(n2)
        rows2, (*act, slope_image, slope_text) = self.spread("gelu", pieces, up)
        if held is not None:
            act[0], held = tie(act[0], held)
        partial = self.collect(act[:1], act[1:], down)
        got = self.ring.scatter(*partial)
        if following is None:
            branch2, y = settle(self.image_rows, 5, None, middle, *partial[:2], *got, modulation, modulation)
            n = None
        else:
            branch2, y, n = settle(self.image_rows, 5, 0, middle, *partial[:2], *got, modulation, following)
        saved = (x, modulation, rows1, kept, mixture, branch1, middle, rows2, (slope_image, slope_text), act, branch2)
        return y, n, saved, held

    def backward_mlp(self, g, db2, saved, weights):
        _, _, up, down = weights
        _, modulation, _, _, _, _, middle, rows2, slopes, act, branch2 = saved
        pieces = self.ring.gather(db2)
        db2, d_pre = self.spread("slope", pieces, down, slopes)
        partial = self.collect(d_pre[:1], d_pre[1:], up)
        got = self.ring.scatter(*partial)
        d_middle, db1, mods = unsettle(
            self.image_rows, 3, 2, middle, g, branch2, *partial[:2], *got, modulation, modulation
        )
        pieces = self.ring.gather(db1)
        return d_middle, mods, pieces, pair_up(rows2, d_pre), pair_up(db2, act)

    def backward_attention(self, d_middle, pieces, saved, below, weights, mask):
        qkv, out, _, _ = weights
        x, modulation, rows1, kept, mixture, branch1, _, _, _, _, _ = saved
        db1, d_mixture = self.spread("", pieces, out)
        d_image, d_text = attention_back(kept, mask, d_mixture)
        partial = self.collect(d_image, d_text, qkv)
        got = self.ring.scatter(*partial)
        g, db2, mods = unsettle(
            self.image_rows,
            0,
            None if below is None else 5,
            x,
            d_middle,
            branch1,
            *partial[:2],
            *got,
            modulation,
            modulation if below is None else below,
        )
        grouped = [(rows1[0], d_image), (rows1[1], d_text)]
        return g, db2, mods, grouped, pair_up(db1, mixture)


def pair_up(rows, values):
    return [(a, [b]) for a, b in zip(rows, values)]


def low(values):
    return [v.astype(LOW) for v in values]


def tie(*values):
    return lax.optimization_barrier(values)


def gather_weight(w):
    return lax.all_gather(w, "dp", axis=1, tiled=True)


def weight_grads(pairs):
    if pairs[0][0][1][0].shape[1] % 128:
        pairs = [[(a, [jnp.concatenate(bs, axis=1)]) for a, bs in pair] for pair in pairs]
    return grad_product(pairs)


def reduce_weight(total):
    return lax.psum_scatter(total, "dp", scatter_dimension=1, tiled=True)


def exchange_sum(parts, axis):
    return jnp.sum(lax.all_to_all(parts, axis, split_axis=0, concat_axis=0, tiled=True), axis=0)


def device_program(
    mp_size,
    image_input,
    text_input,
    timesteps,
    key_mask,
    mod_weight,
    qkv_weight,
    out_weight,
    up_weight,
    down_weight,
    image_cotangent,
    text_cotangent,
):
    seqs = key_mask.shape[0]
    assert seqs == 2
    width = image_input.shape[1]
    ring = Ring(mp_size)
    half = mp_size // 2
    side = lax.axis_index("mp") // half
    swap = [(i, (i + half) % mp_size) for i in range(mp_size)]
    ri, rt = image_input.shape[0] // 2, text_input.shape[0] // 2
    here = side == 0

    def deal(image, text):
        pieces = [jnp.concatenate([image[p * ri : p * ri + ri], text[p * rt : p * rt + rt]], axis=0) for p in range(2)]
        got = lax.ppermute(jnp.where(here, pieces[1], pieces[0]), "mp", swap)
        return [jnp.where(here, pieces[0], got).astype(F32), jnp.where(here, got, pieces[1]).astype(F32)]

    def undeal(rows):
        got = lax.ppermute(jnp.where(here, rows[1], rows[0]), "mp", swap)
        pieces = [jnp.where(here, rows[0], got), jnp.where(here, got, rows[1])]
        return (
            jnp.concatenate([piece[:ri] for piece in pieces], axis=0),
            jnp.concatenate([piece[ri:] for piece in pieces], axis=0),
        )

    condition = conditioning(timesteps, width).astype(LOW)
    depth = mod_weight.shape[2]
    own_condition = lax.dynamic_slice_in_dim(condition, lax.axis_index("dp") * depth, depth, axis=1)
    partial = jnp.einsum("nd,lsdkc->nlskc", own_condition, mod_weight, preferred_element_type=F32)
    columns = mod_weight.shape[4]
    own_mod = exchange_sum(partial.reshape(-1, seqs * LAYERS * 12, columns), "dp")
    modulation = lax.all_gather(own_mod, "mp", axis=0)
    modulation = jnp.swapaxes(modulation, 0, 1).reshape(seqs, LAYERS, 2, 6, width)

    owners = jnp.array(ring.owners(), dtype=jnp.int32)[lax.axis_index("mp")]
    segments = (owners % half) * 2 + owners // half
    masks = jnp.take(key_mask.reshape(seqs, mp_size, rt), segments, axis=1).reshape(seqs, -1)

    weights = []
    for l in range(LAYERS):
        weights.append(
            (
                gather_weight(jnp.swapaxes(qkv_weight[l], 1, 2).reshape(2, qkv_weight.shape[3], -1)),
                gather_weight(jnp.swapaxes(out_weight[l], 1, 2)),
                gather_weight(up_weight[l]),
                gather_weight(jnp.swapaxes(down_weight[l], 1, 2)),
            )
        )

    keep = (jnp.arange(ri + rt) < ri)[:, None]
    step = Step(ring, ri, rt, keep)
    rows = deal(image_input, text_input)
    upstream = deal(image_cotangent, text_cotangent)
    saved = []
    mods = [[modulation[s, l] for l in range(LAYERS)] + [None] for s in range(seqs)]
    ready = [low([step.start(rows[s], mods[s][0])])[0] for s in range(seqs)]
    last = LAYERS - 1
    db2 = [low([step.pick(mods[s][last], 5) * upstream[s]])[0] for s in range(seqs)]
    for l in range(LAYERS):
        done = [
            step.forward(rows[s], ready[s], mods[s][l], mods[s][l + 1], weights[l], masks[s], None if l else db2[s])
            for s in range(seqs)
        ]
        rows, ready = [d[0] for d in done], [d[1] for d in done]
        saved.append([d[2] for d in done])
        if l == 0:
            db2 = [d[3] for d in done]
    image_output, text_output = undeal(rows)

    reduced, mod_rows = [None] * LAYERS, [None] * LAYERS
    for l in reversed(range(LAYERS)):
        mlp = [step.backward_mlp(upstream[s], db2[s], saved[l][s], weights[l]) for s in range(seqs)]
        down_total = weight_grads([m[4] for m in mlp])
        up_total = weight_grads([m[3] for m in mlp])
        db1 = [m[2] for m in mlp]
        grad_down = reduce_weight(down_total)
        grad_up = reduce_weight(up_total)
        if l < last:
            db1[1], above_up, above_down = tie(db1[1], reduced[l + 1][2], reduced[l + 1][3])
            reduced[l + 1][2:] = [above_up, above_down]
        att = [
            step.backward_attention(mlp[s][0], db1[s], saved[l][s], mods[s][l - 1] if l else None, weights[l], masks[s])
            for s in range(seqs)
        ]
        out_total = weight_grads([a[4] for a in att])
        qkv_total = weight_grads([a[3] for a in att])
        upstream, db2 = [a[0] for a in att], [a[1] for a in att]
        if l:
            db2[1], out_total, qkv_total = tie(db2[1], out_total, qkv_total)
        grad_out = reduce_weight(out_total)
        grad_qkv = reduce_weight(qkv_total)
        mod_rows[l] = jnp.stack([jnp.concatenate([att[s][2], mlp[s][1]], axis=1) for s in range(seqs)])
        reduced[l] = [grad_qkv, grad_out, grad_up, grad_down]
    image_grad, text_grad = undeal(upstream)
    reduced = [[r.astype(F32) for r in layer] for layer in reduced]

    mod_rows = jnp.stack(mod_rows, axis=1).reshape(-1, mp_size, columns)
    mod_sums = exchange_sum(jnp.swapaxes(mod_rows, 0, 1).reshape(mp_size, -1, columns), "mp")
    all_mods = lax.all_gather(mod_sums, "dp", axis=0).reshape(-1, LAYERS, 2, 6, columns)
    grad_mod = jnp.einsum("nd,nlskc->lsdkc", own_condition.astype(F32), all_mods, precision=lax.Precision.HIGHEST)
    grad_qkv = jnp.stack(
        [jnp.swapaxes(r[0].reshape(2, -1, 3, columns), 1, 2) for r in reduced]
    )
    return (
        image_output,
        text_output,
        image_grad,
        text_grad,
        grad_mod,
        grad_qkv,
        jnp.stack([jnp.swapaxes(r[1], 1, 2) for r in reduced]),
        jnp.stack([r[2] for r in reduced]),
        jnp.stack([jnp.swapaxes(r[3], 1, 2) for r in reduced]),
    )


def solution(mesh):
    rows = P(("dp", "mp"), None)
    grads = (
        P(None, None, "dp", None, "mp"),
        P(None, None, None, "dp", "mp"),
        P(None, None, "mp", "dp"),
        P(None, None, "dp", "mp"),
        P(None, None, "mp", "dp"),
    )

    def program(*arrays):
        return device_program(mesh.shape["mp"], *arrays)

    return jax.shard_map(
        program,
        mesh=mesh,
        in_specs=(rows, rows, P(), P("dp", None)) + grads + (rows, rows),
        out_specs=(rows, rows, rows, rows) + grads,
        check_vma=False,
    )
```

```python
import functools
import math

import jax
import jax.numpy as jnp
from jax import lax
from jax.experimental import pallas as pl
from jax.experimental.pallas import tpu as pltpu
from jax.sharding import PartitionSpec as P


HEAD_DIM = 64
LAYERS = 2
EPSILON = 1e-06
LOW = jnp.bfloat16
F32 = jnp.float32
PAIR=128
NT=(((1,),(1,)),((),()))
TN=(((0,),(0,)),((),()))
NN=(((1,),(0,)),((),()))


def dot(a,b,dims):
    return lax.dot_general(a,b,dims,preferred_element_type=jnp.float32)


def attn_fwd_kernel(scale,qb,mask_ref,qi,ki,vi,qt,kt,vt,oi,ot,li,lt):
    low = lax.broadcasted_iota(jnp.int32,(1,PAIR),1)<HEAD_DIM
    live = mask_ref[0:1,:]>0
    k_img,k_txt,v_img,v_txt=ki[...],kt[...],vi[...],vt[...]

    def block(q,store):
        q=q*jnp.asarray(scale,q.dtype)
        outs=[];lses=[]
        for h in range(2):
            keep = low if h==0 else jnp.logical_not(low)
            qm=jnp.where(keep,q,jnp.zeros_like(q))
            si=dot(qm,k_img,NT); st=jnp.where(live,dot(qm,k_txt,NT),-1e30)
            m=jnp.maximum(jnp.max(si,axis=-1,keepdims=True),jnp.max(st,axis=-1,keepdims=True))
            pi=jnp.exp(si-m); pt=jnp.exp(st-m)
            l=jnp.sum(pi,axis=-1,keepdims=True)+jnp.sum(pt,axis=-1,keepdims=True)
            o=dot(pi.astype(jnp.bfloat16),v_img,NN)+dot(pt.astype(jnp.bfloat16),v_txt,NN)
            outs.append(o/l); lses.append(m+jnp.log(l))
        store(jnp.where(low,outs[0],outs[1]).astype(jnp.bfloat16), jnp.where(low,lses[0],lses[1]))

    nb=qi.shape[0]//qb

    def body(b,c):
        r=pl.ds(pl.multiple_of(b*qb,qb),qb)

        def store(o,l):
            oi[r,:]=o; li[r,:]=l

        block(qi[r,:],store)
        return c

    lax.fori_loop(0,nb,body,0)

    def store(o,l):
        ot[...]=o; lt[...]=l

    block(qt[...],store)


def attn_fwd(img,txt,mask,qb=256):
    ri,c3=img.shape; rt=txt.shape[0]; c=c3//3; np_=c//PAIR
    spec=lambda r,off: pl.BlockSpec((r,PAIR),lambda j,off=off:(0,j+off*np_))
    f=pl.pallas_call(functools.partial(attn_fwd_kernel,HEAD_DIM**-0.5,qb),
        grid=(np_,),
        in_specs=[pl.BlockSpec((8,rt),lambda j:(0,0))]+[spec(ri,o) for o in range(3)]+[spec(rt,o) for o in range(3)],
        out_specs=[spec(ri,0),spec(rt,0),spec(ri,0),spec(rt,0)],
        out_shape=[jax.ShapeDtypeStruct((ri,c),jnp.bfloat16),jax.ShapeDtypeStruct((rt,c),jnp.bfloat16),
                   jax.ShapeDtypeStruct((ri,c),jnp.float32),jax.ShapeDtypeStruct((rt,c),jnp.float32)],
        compiler_params=pltpu.CompilerParams(vmem_limit_bytes=56<<20),
        cost_estimate=pl.CostEstimate(flops=4*(ri+rt)**2*c,bytes_accessed=(ri+rt)*c*12,transcendentals=(ri+rt)**2*c//HEAD_DIM),
        name="attn_fwd")
    return f(mask,img,img,img,txt,txt,txt)


def attn_bwd_kernel(scale,qb,mask_ref,qi,ki,vi,qt,kt,vt,oi,ot,li,lt,gi,gt,dqi,dki,dvi,dqt,dkt,dvt,aki,avi,akt,avt):
    low = lax.broadcasted_iota(jnp.int32,(1,PAIR),1)<HEAD_DIM
    live = mask_ref[:,0:1]>0
    k_img,k_txt,v_img,v_txt=ki[...],kt[...],vi[...],vt[...]
    for a in (aki,avi,akt,avt): a[...]=jnp.zeros_like(a)
    keeps=[low,jnp.logical_not(low)]
    kim=[jnp.where(k,k_img,jnp.zeros_like(k_img)) for k in keeps]
    ktm=[jnp.where(k,k_txt,jnp.zeros_like(k_txt)) for k in keeps]

    def block(q,o,l,g,store):
        q=q*jnp.asarray(scale,q.dtype)
        lT=l.T
        dT=(g.astype(jnp.float32)*o.astype(jnp.float32)).T
        dq=None
        for h in range(2):
            qm=jnp.where(keeps[h],q,jnp.zeros_like(q)); gm=jnp.where(keeps[h],g,jnp.zeros_like(g))
            lr=lT[h*HEAD_DIM:h*HEAD_DIM+1,:]
            dr=jnp.sum(dT[h*HEAD_DIM:(h+1)*HEAD_DIM,:],axis=0,keepdims=True)
            pi=jnp.exp(dot(k_img,qm,NT)-lr)
            pt=jnp.exp(jnp.where(live,dot(k_txt,qm,NT),-1e30)-lr)
            avi[...]+=dot(pi.astype(jnp.bfloat16),gm,NN)
            avt[...]+=dot(pt.astype(jnp.bfloat16),gm,NN)
            si=(pi*(dot(v_img,gm,NT)-dr)).astype(jnp.bfloat16)
            st=(pt*(dot(v_txt,gm,NT)-dr)).astype(jnp.bfloat16)
            aki[...]+=dot(si,qm,NN)
            akt[...]+=dot(st,qm,NN)
            d=dot(si,kim[h],TN)+dot(st,ktm[h],TN)
            dq=d if dq is None else dq+d
        store((dq*scale).astype(jnp.bfloat16))

    nb=qi.shape[0]//qb

    def body(b,c):
        r=pl.ds(pl.multiple_of(b*qb,qb),qb)

        def store(v): dqi[r,:]=v

        block(qi[r,:],oi[r,:],li[r,:],gi[r,:],store)
        return c

    lax.fori_loop(0,nb,body,0)

    def store(v): dqt[...]=v

    block(qt[...],ot[...],lt[...],gt[...],store)
    dki[...]=aki[...].astype(jnp.bfloat16); dvi[...]=avi[...].astype(jnp.bfloat16)
    dkt[...]=akt[...].astype(jnp.bfloat16); dvt[...]=avt[...].astype(jnp.bfloat16)


def attn_bwd(img,txt,mask,oi,ot,li,lt,gi,gt,qb=256):
    ri,c3=img.shape; rt=txt.shape[0]; c=c3//3; np_=c//PAIR
    spec=lambda r,off=0: pl.BlockSpec((r,PAIR),lambda j,off=off:(0,j+off*np_))
    f=pl.pallas_call(functools.partial(attn_bwd_kernel,HEAD_DIM**-0.5,qb),
        grid=(np_,),
        in_specs=[pl.BlockSpec((rt,128),lambda j:(0,0))]+[spec(ri,o) for o in range(3)]+[spec(rt,o) for o in range(3)]
            +[spec(ri),spec(rt)]*3,
        out_specs=[spec(ri)]*3+[spec(rt)]*3,
        out_shape=[jax.ShapeDtypeStruct((ri,c),jnp.bfloat16)]*3+[jax.ShapeDtypeStruct((rt,c),jnp.bfloat16)]*3,
        scratch_shapes=[pltpu.VMEM((ri,PAIR),jnp.float32)]*2+[pltpu.VMEM((rt,PAIR),jnp.float32)]*2,
        compiler_params=pltpu.CompilerParams(vmem_limit_bytes=56<<20),
        cost_estimate=pl.CostEstimate(flops=10*(ri+rt)**2*c,bytes_accessed=(ri+rt)*c*26,transcendentals=(ri+rt)**2*c//HEAD_DIM),
        name="attn_bwd")
    return f(mask,img,img,img,txt,txt,txt,oi,ot,li,lt,gi,gt)


def attention(img, txt, mask):
    c = img.shape[1] // 3
    pad = -c % PAIR
    if pad:
        img, txt = (jnp.pad(a.reshape(-1, 3, c), ((0, 0), (0, 0), (0, pad))).reshape(-1, 3 * (c + pad)) for a in (img, txt))
    mask_rows = jnp.broadcast_to(mask[None, :], (8, mask.shape[0]))
    oi, ot, li, lt = attn_fwd(img, txt, mask_rows, query_block(img.shape[0]))
    return (oi[:, :c], ot[:, :c]), (img, txt, oi, ot, li, lt)


def attention_back(kept, mask, grads):
    img, txt, oi, ot, li, lt = kept
    c = grads[0].shape[1]
    pad = oi.shape[1] - c
    gi, gt = (jnp.pad(g, ((0, 0), (0, pad))) for g in grads) if pad else grads
    mask_columns = jnp.broadcast_to(mask[:, None], (mask.shape[0], 128))
    out = attn_bwd(img, txt, mask_columns, oi, ot, li, lt, gi, gt, query_block(img.shape[0]))
    return tuple([piece[:, :c] for piece in part] for part in (out[:3], out[3:]))


def query_block(rows):
    return 256 if rows % 256 == 0 else rows


def conditioning(steps, width):
    half = width // 2
    frequency = jnp.exp(-math.log(10000.0) * jnp.arange(half, dtype=F32) / half)
    phases = steps.astype(F32)[..., None] * frequency
    embedded = jnp.concatenate([jnp.cos(phases), jnp.sin(phases)], axis=-1)
    return embedded / (1.0 + jnp.exp(-embedded))


def normed(v):
    centred = v - jnp.mean(v, axis=-1, keepdims=True)
    r = lax.rsqrt(jnp.mean(centred * centred, axis=-1, keepdims=True) + EPSILON)
    return centred * r, r


class Ring:
    def __init__(self, size):
        self.size = size
        half = size // 2
        self.order = list(range(half)) + list(range(size - 1, half - 1, -1))
        self.up = [(self.order[i], self.order[(i + 1) % size]) for i in range(size)]
        self.down = [(self.order[i], self.order[(i - 1) % size]) for i in range(size)]

    def offsets(self):
        out = [0]
        for t in range(1, self.size // 2):
            out += [-t, t]
        return out + [self.size // 2]

    def owners(self):
        place = {device: i for i, device in enumerate(self.order)}
        return [
            [self.order[(place[device] + offset) % self.size] for offset in self.offsets()]
            for device in range(self.size)
        ]

    def shift(self, up, down):
        return lax.ppermute(up, "mp", self.up), lax.ppermute(down, "mp", self.down)

    def gather(self, x):
        cut = cut_of(x.shape[0])
        blocks, a, b = [x], x, x
        for _ in range(1, self.size // 2):
            a, b = self.shift(a, b)
            blocks += [a, b]
        first, second = self.shift(a[:cut], b[cut:])
        return blocks, (first, second)

    def scatter(self, image, text, first, second):
        rows, extra = image.shape[0] // self.size, text.shape[0] // self.size
        up, down = self.shift(first, second)
        half = self.size // 2
        if half == 1:
            full = jnp.concatenate([up, down], axis=0)
            return full, jnp.zeros_like(full)
        for t in range(half - 1, 0, -1):
            ahead, behind = ring_add(image, text, up, down, 2 * t, 2 * t - 1, rows, extra, t == half - 1)
            up, down = self.shift(ahead, behind)
        return up, down


def cut_of(rows):
    return rows // 32 * 16


def ring_add_kernel(halves, ia, ib, text, up, down, ahead, behind, ka, kb):
    rows, cut = ia.shape[0], up.shape[0]
    extra = ahead.shape[0] - rows
    wide = lambda v: v.astype(F32)
    ta = text[ka * extra : (ka + 1) * extra, :]
    tb = text[kb * extra : (kb + 1) * extra, :]
    if halves:
        ahead[:cut, :] = (wide(ia[:cut, :]) + wide(up[...])).astype(LOW)
        ahead[cut:rows, :] = ia[cut:, :]
        ahead[rows:, :] = ta
        behind[:cut, :] = ib[:cut, :]
        behind[cut:rows, :] = (wide(ib[cut:, :]) + wide(down[: rows - cut, :])).astype(LOW)
        behind[rows:, :] = (wide(tb) + wide(down[rows - cut :, :])).astype(LOW)
    else:
        for out, image, words, got in ((ahead, ia, ta, up), (behind, ib, tb, down)):
            out[:rows, :] = (wide(image[...]) + wide(got[:rows, :])).astype(LOW)
            out[rows:, :] = (wide(words) + wide(got[rows:, :])).astype(LOW)


def whole(a):
    return pl.BlockSpec(a.shape, lambda i: (0,) * len(a.shape))


def ring_add(image, text, up, down, ka, kb, rows, extra, halves):
    width = image.shape[1]
    out = jax.ShapeDtypeStruct((rows + extra, width), LOW)
    return pl.pallas_call(
        lambda *refs: ring_add_kernel(halves, *refs, ka, kb),
        grid=(1,),
        in_specs=[
            pl.BlockSpec((rows, width), lambda i: (ka, 0)),
            pl.BlockSpec((rows, width), lambda i: (kb, 0)),
            whole(text),
            whole(up),
            whole(down),
        ],
        out_specs=[whole(out)] * 2,
        out_shape=[out] * 2,
        cost_estimate=pl.CostEstimate(flops=rows * width, bytes_accessed=rows * width * 10, transcendentals=0),
        name="ring_add",
    )(image, image, text, up, down)


def row_loop(rows, extra, body):
    for stream, start, count in ((0, 0, rows), (1, rows, extra)):
        chunk = 16 if count % 16 == 0 else 8 if count % 8 == 0 else count
        if chunk == count:
            body(stream, pl.ds(start, count), pl.ds(0, count))
            continue

        def one(i, carry, stream=stream, start=start, chunk=chunk):
            off = pl.multiple_of(i * chunk, chunk)
            body(stream, pl.ds(pl.multiple_of(start + off, 8), chunk), pl.ds(off, chunk))
            return carry

        lax.fori_loop(0, count // chunk, one, 0)


def mean(v):
    return jnp.mean(v, axis=-1, keepdims=True)


def settle_kernel(rows, gate, norm, x, own, text, up, down, gates, norms, branch, y, n):
    def body(s, r, q):
        mine = own if s == 0 else text
        b = mine[q, :].astype(F32) + up[r, :].astype(F32) + down[r, :].astype(F32)
        branch[r, :] = b.astype(LOW)
        v = x[r, :] + gates[s, gate : gate + 1, :] * b
        y[r, :] = v.astype(y.dtype)
        if norm is not None:
            centred = v - mean(v)
            unit = centred * lax.rsqrt(mean(centred * centred) + EPSILON)
            n[r, :] = (unit * (1.0 + norms[s, norm + 1 : norm + 2, :]) + norms[s, norm : norm + 1, :]).astype(LOW)

    row_loop(rows, x.shape[0] - rows, body)


def settle(rows, gate, norm, x, image, text, up, down, gates, norms):
    height, width = x.shape
    shape = lambda kind: jax.ShapeDtypeStruct((height, width), kind)
    outs = [shape(LOW), shape(LOW if norm is None else F32)] + ([] if norm is None else [shape(LOW)])
    kernel = functools.partial(settle_kernel, rows, gate, norm)
    if norm is None:
        kernel = lambda *refs: settle_kernel(rows, gate, None, *refs, None)
    return pl.pallas_call(
        kernel,
        grid=(1,),
        in_specs=[whole(x), pl.BlockSpec((rows, width), lambda i: (0, 0))]
        + [whole(a) for a in (text, up, down, gates, norms)],
        out_specs=[whole(o) for o in outs],
        out_shape=outs,
        compiler_params=pltpu.CompilerParams(vmem_limit_bytes=40 << 20),
        cost_estimate=pl.CostEstimate(flops=20 * height * width, bytes_accessed=18 * height * width, transcendentals=0),
        name="settle",
    )(x, image, text, up, down, gates, norms)


def unsettle_kernel(rows, norm, gate, x, g, branch, own, text, up, down, norms, gates, d, low_out, sums):
    sums[...] = jnp.zeros_like(sums)

    def body(s, r, q):
        mine = own if s == 0 else text
        dn = mine[q, :].astype(F32) + up[r, :].astype(F32) + down[r, :].astype(F32)
        v, upstream = x[r, :], g[r, :]
        centred = v - mean(v)
        inverse = lax.rsqrt(mean(centred * centred) + EPSILON)
        n = centred * inverse
        e = dn * (1.0 + norms[s, norm + 1 : norm + 2, :])
        total = upstream + inverse * (e - mean(e) - n * mean(e * n))
        d[r, :] = total
        if gate is not None:
            low_out[r, :] = (gates[s, gate : gate + 1, :] * total).astype(LOW)
        for k, term in enumerate((dn, dn * n, upstream * branch[r, :].astype(F32))):
            sums[s * 3 + k : s * 3 + k + 1, :] += jnp.sum(term, axis=0, keepdims=True)

    row_loop(rows, x.shape[0] - rows, body)


def unsettle(rows, norm, gate, x, g, branch, image, text, up, down, norms, gates):
    height, width = x.shape
    outs = [jax.ShapeDtypeStruct((height, width), F32)]
    if gate is not None:
        outs.append(jax.ShapeDtypeStruct((height, width), LOW))
    outs.append(jax.ShapeDtypeStruct((8, width), F32))
    kernel = functools.partial(unsettle_kernel, rows, norm, gate)
    if gate is None:
        kernel = lambda *refs: unsettle_kernel(rows, norm, None, *refs[:-1], None, refs[-1])
    got = pl.pallas_call(
        kernel,
        grid=(1,),
        in_specs=[whole(x), whole(g), whole(branch), pl.BlockSpec((rows, width), lambda i: (0, 0))]
        + [whole(a) for a in (text, up, down, norms, gates)],
        out_specs=[whole(o) for o in outs],
        out_shape=outs,
        compiler_params=pltpu.CompilerParams(vmem_limit_bytes=40 << 20),
        cost_estimate=pl.CostEstimate(flops=40 * height * width, bytes_accessed=24 * height * width, transcendentals=0),
        name="unsettle",
    )(x, g, branch, image, text, up, down, norms, gates)
    sums = got[-1][:6].reshape(2, 3, width)
    return got[0], (got[1] if gate is not None else None), sums


PARAMS = pltpu.CompilerParams(vmem_limit_bytes=58 << 20)


def tile_of(columns):
    return 384 if columns % 384 == 0 else columns


def halves_of(rows):
    step = rows // 2 if rows % 32 == 0 and rows > 512 else rows
    return [slice(i, i + step) for i in range(0, rows, step)]


def spread_kernel(mode, count, *refs):
    blocks, (first, second, wi, wt), rest = refs[:count], refs[count : count + 4], refs[count + 4 :]
    slopes, rest = (rest[:2], rest[2:]) if mode == "slope" else (None, rest)
    ri, rt, out = rest[0], rest[1], rest[2:]

    @pl.when(pl.program_id(0) == 0)
    def _():
        r, e, cut = ri.shape[0] // (count + 1), rt.shape[0] // (count + 1), first.shape[0]
        for k, block in enumerate(blocks):
            ri[k * r : (k + 1) * r, :] = block[:r, :]
            rt[k * e : (k + 1) * e, :] = block[r:, :]
        ri[count * r : count * r + cut, :] = first[...]
        ri[count * r + cut :, :] = second[: r - cut, :]
        rt[count * e :, :] = second[r - cut :, :]

    for s, (rows, w) in enumerate(((ri, wi), (rt, wt))):
        for part in halves_of(rows.shape[0]):
            v = dot(rows[part, :], w[...], NN)
            if mode == "gelu":
                t = jnp.tanh(0.7978845608028654 * (v + 0.044715 * v * v * v))
                half = 0.5 * (1.0 + t)
                out[s][part, :] = (v * half).astype(LOW)
                bend = 0.7978845608028654 * (1.0 + 0.134145 * v * v)
                out[2 + s][part, :] = (half + 0.5 * v * (1.0 - t * t) * bend).astype(LOW)
            elif mode == "slope":
                out[s][part, :] = (v * slopes[s][part, :].astype(F32)).astype(LOW)
            else:
                out[s][part, :] = v.astype(LOW)


def spread_product(mode, rows, pieces, weight, slopes=()):
    blocks, (first, second) = pieces
    count = len(blocks)
    size = count + 1
    height, depth = blocks[0].shape
    columns = weight.shape[2]
    tile = tile_of(columns)
    heights = (rows * size, (height - rows) * size)
    wide = [pl.BlockSpec((h, tile), lambda j: (0, j)) for h in heights]
    products = 4 if mode == "gelu" else 2
    return pl.pallas_call(
        functools.partial(spread_kernel, mode, count),
        grid=(columns // tile,),
        in_specs=[whole(a) for a in (*blocks, first, second)]
        + [pl.BlockSpec((None, depth, tile), lambda j, s=s: (s, 0, j)) for s in range(2)]
        + (wide if slopes else []),
        out_specs=[pl.BlockSpec((h, depth), lambda j: (0, 0)) for h in heights] + wide * (products // 2),
        out_shape=[jax.ShapeDtypeStruct((h, depth), LOW) for h in heights]
        + [jax.ShapeDtypeStruct((h, columns), LOW) for h in heights] * (products // 2),
        compiler_params=PARAMS,
        cost_estimate=pl.CostEstimate(
            flops=2 * sum(heights) * depth * columns,
            bytes_accessed=4 * depth * columns + 4 * sum(heights) * (depth + columns),
            transcendentals=0,
        ),
        name="spread",
    )(*blocks, first, second, weight, weight, *slopes)


def collect_kernel(count, size, *refs):
    xs = (refs[:count], refs[count : 2 * count])
    ws = (refs[2 * count : 3 * count], refs[3 * count : 4 * count])
    pi, pt, first, second = refs[4 * count :]
    for out, x, w in zip((pi, pt), *zip(*((xs[s], ws[s]) for s in range(2)))):
        for part in halves_of(out.shape[0]):
            out[part, :] = sum(dot(a[part, :], b[...], NT) for a, b in zip(x, w)).astype(LOW)
    r, e, cut = pi.shape[0] // size, pt.shape[0] // size, first.shape[0]
    far = (size - 1) * r
    first[...] = pi[far : far + cut, :]
    second[: r - cut, :] = pi[far + cut :, :]
    second[r - cut :, :] = pt[(size - 1) * e :, :]


def collect_product(size, image, text, weight):
    count, group = len(image), image[0].shape[1]
    height, extra = image[0].shape[0], text[0].shape[0]
    width = weight.shape[1]
    tile = tile_of(width)
    cut = cut_of((height + extra) // size)
    rest = (height + extra) // size - cut
    outs = (height, extra, cut, rest)
    return pl.pallas_call(
        functools.partial(collect_kernel, count, size),
        grid=(width // tile,),
        in_specs=[whole(a) for a in (*image, *text)]
        + [pl.BlockSpec((None, tile, group), lambda j, s=s, k=k: (s, j, k)) for s in range(2) for k in range(count)],
        out_specs=[pl.BlockSpec((h, tile), lambda j: (0, j)) for h in outs],
        out_shape=[jax.ShapeDtypeStruct((h, width), LOW) for h in outs],
        compiler_params=PARAMS,
        cost_estimate=pl.CostEstimate(
            flops=2 * (height + extra) * width * group * count,
            bytes_accessed=4 * width * group * count + 2 * (height + extra) * (width + group * count),
            transcendentals=0,
        ),
        name="collect",
    )(*image, *text, *([weight] * (2 * count)))


def grad_kernel(seqs, count, *refs):
    out = refs[-1]
    per = 2 * (1 + count)
    for s in range(2):
        for k in range(count):
            total = None
            for q in range(seqs):
                mine = refs[q * per + s * (1 + count) : q * per + (s + 1) * (1 + count)]
                v = dot(mine[0][...], mine[1 + k][...], TN)
                total = v if total is None else total + v
            columns = total.shape[1]
            out[s, :, k * columns : (k + 1) * columns] = total.astype(LOW)


def grad_product(pairs):
    seqs, count = len(pairs), len(pairs[0][0][1])
    width = pairs[0][0][0].shape[1]
    columns = count * pairs[0][0][1][0].shape[1]
    tile = 256 if width % 256 == 0 else width
    arrays, specs, rows = [], [], 0
    for pair in pairs:
        for a, bs in pair:
            arrays += [a, *bs]
            specs += [pl.BlockSpec((a.shape[0], tile), lambda i: (0, i))] + [whole(b) for b in bs]
            rows += a.shape[0]
    return pl.pallas_call(
        functools.partial(grad_kernel, seqs, count),
        grid=(width // tile,),
        in_specs=specs,
        out_specs=pl.BlockSpec((2, tile, columns), lambda i: (0, i, 0)),
        out_shape=jax.ShapeDtypeStruct((2, width, columns), LOW),
        compiler_params=PARAMS,
        cost_estimate=pl.CostEstimate(
            flops=2 * rows * width * columns,
            bytes_accessed=4 * width * columns + 2 * rows * (width + columns),
            transcendentals=0,
        ),
        name="grad",
    )(*arrays)


class Step:
    def __init__(self, ring, image_rows, text_rows, keep):
        self.ring, self.image_rows, self.text_rows, self.keep = ring, image_rows, text_rows, keep

    def pick(self, modulation, member):
        return jnp.where(self.keep, modulation[0, member][None, :], modulation[1, member][None, :])

    def spread(self, mode, pieces, weight, slopes=()):
        got = spread_product(mode, self.image_rows, pieces, weight, slopes)
        return got[:2], got[2:]

    def collect(self, image, text, weight):
        if image[0].shape[1] % 128:
            image, text = ([jnp.concatenate(a, axis=1)] for a in (image, text))
        return collect_product(self.ring.size, image, text, weight)

    def start(self, x, modulation):
        return normed(x)[0] * (1.0 + self.pick(modulation, 1)) + self.pick(modulation, 0)

    def forward(self, x, n1, modulation, following, weights, mask):
        qkv, out, up, down = weights
        pieces = self.ring.gather(n1)
        rows1, proj = self.spread("", pieces, qkv)
        mixture, kept = attention(proj[0], proj[1], mask)
        partial = self.collect(mixture[:1], mixture[1:], out)
        got = self.ring.scatter(*partial)
        branch1, middle, n2 = settle(self.image_rows, 2, 3, x, *partial[:2], *got, modulation, modulation)
        pieces = self.ring.gather(n2)
        rows2, (*act, slope_image, slope_text) = self.spread("gelu", pieces, up)
        partial = self.collect(act[:1], act[1:], down)
        got = self.ring.scatter(*partial)
        if following is None:
            branch2, y = settle(self.image_rows, 5, None, middle, *partial[:2], *got, modulation, modulation)
            n = None
        else:
            branch2, y, n = settle(self.image_rows, 5, 0, middle, *partial[:2], *got, modulation, following)
        saved = (x, modulation, rows1, kept, mixture, branch1, middle, rows2, (slope_image, slope_text), act, branch2)
        return y, n, saved

    def backward_mlp(self, g, db2, saved, weights):
        _, _, up, down = weights
        _, modulation, _, _, _, _, middle, rows2, slopes, act, branch2 = saved
        pieces = self.ring.gather(db2)
        db2, d_pre = self.spread("slope", pieces, down, slopes)
        partial = self.collect(d_pre[:1], d_pre[1:], up)
        got = self.ring.scatter(*partial)
        d_middle, db1, mods = unsettle(
            self.image_rows, 3, 2, middle, g, branch2, *partial[:2], *got, modulation, modulation
        )
        pieces = self.ring.gather(db1)
        return d_middle, mods, pieces, pair_up(rows2, d_pre), pair_up(db2, act)

    def backward_attention(self, d_middle, pieces, saved, below, weights, mask):
        qkv, out, _, _ = weights
        x, modulation, rows1, kept, mixture, branch1, _, _, _, _, _ = saved
        db1, d_mixture = self.spread("", pieces, out)
        d_image, d_text = attention_back(kept, mask, d_mixture)
        partial = self.collect(d_image, d_text, qkv)
        got = self.ring.scatter(*partial)
        g, db2, mods = unsettle(
            self.image_rows,
            0,
            None if below is None else 5,
            x,
            d_middle,
            branch1,
            *partial[:2],
            *got,
            modulation,
            modulation if below is None else below,
        )
        grouped = [(rows1[0], d_image), (rows1[1], d_text)]
        return g, db2, mods, grouped, pair_up(db1, mixture)


def pair_up(rows, values):
    return [(a, [b]) for a, b in zip(rows, values)]


def low(values):
    return [v.astype(LOW) for v in values]


def tie(*values):
    return lax.optimization_barrier(values)


def gather_weight(w):
    return lax.all_gather(w, "dp", axis=1, tiled=True)


def weight_grads(pairs):
    if pairs[0][0][1][0].shape[1] % 128:
        pairs = [[(a, [jnp.concatenate(bs, axis=1)]) for a, bs in pair] for pair in pairs]
    return grad_product(pairs)


def reduce_weight(total):
    return lax.psum_scatter(total, "dp", scatter_dimension=1, tiled=True)


def exchange_sum(parts, axis):
    return jnp.sum(lax.all_to_all(parts, axis, split_axis=0, concat_axis=0, tiled=True), axis=0)


def device_program(
    mp_size,
    image_input,
    text_input,
    timesteps,
    key_mask,
    mod_weight,
    qkv_weight,
    out_weight,
    up_weight,
    down_weight,
    image_cotangent,
    text_cotangent,
):
    seqs = key_mask.shape[0]
    assert seqs == 2
    width = image_input.shape[1]
    ring = Ring(mp_size)
    half = mp_size // 2
    side = lax.axis_index("mp") // half
    swap = [(i, (i + half) % mp_size) for i in range(mp_size)]
    ri, rt = image_input.shape[0] // 2, text_input.shape[0] // 2
    here = side == 0

    def deal(image, text):
        pieces = [jnp.concatenate([image[p * ri : p * ri + ri], text[p * rt : p * rt + rt]], axis=0) for p in range(2)]
        got = lax.ppermute(jnp.where(here, pieces[1], pieces[0]), "mp", swap)
        return [jnp.where(here, pieces[0], got).astype(F32), jnp.where(here, got, pieces[1]).astype(F32)]

    def undeal(rows):
        got = lax.ppermute(jnp.where(here, rows[1], rows[0]), "mp", swap)
        pieces = [jnp.where(here, rows[0], got), jnp.where(here, got, rows[1])]
        return (
            jnp.concatenate([piece[:ri] for piece in pieces], axis=0),
            jnp.concatenate([piece[ri:] for piece in pieces], axis=0),
        )

    condition = conditioning(timesteps, width).astype(LOW)
    depth = mod_weight.shape[2]
    own_condition = lax.dynamic_slice_in_dim(condition, lax.axis_index("dp") * depth, depth, axis=1)
    partial = jnp.einsum("nd,lsdkc->nlskc", own_condition, mod_weight, preferred_element_type=F32)
    columns = mod_weight.shape[4]
    own_mod = exchange_sum(partial.reshape(-1, seqs * LAYERS * 12, columns), "dp")
    modulation = lax.all_gather(own_mod, "mp", axis=0)
    modulation = jnp.swapaxes(modulation, 0, 1).reshape(seqs, LAYERS, 2, 6, width)

    owners = jnp.array(ring.owners(), dtype=jnp.int32)[lax.axis_index("mp")]
    segments = (owners % half) * 2 + owners // half
    masks = jnp.take(key_mask.reshape(seqs, mp_size, rt), segments, axis=1).reshape(seqs, -1)

    weights = []
    for l in range(LAYERS):
        weights.append(
            (
                gather_weight(jnp.swapaxes(qkv_weight[l], 1, 2).reshape(2, qkv_weight.shape[3], -1)),
                gather_weight(jnp.swapaxes(out_weight[l], 1, 2)),
                gather_weight(up_weight[l]),
                gather_weight(jnp.swapaxes(down_weight[l], 1, 2)),
            )
        )

    keep = (jnp.arange(ri + rt) < ri)[:, None]
    step = Step(ring, ri, rt, keep)
    rows = deal(image_input, text_input)
    upstream = deal(image_cotangent, text_cotangent)
    saved = []
    mods = [[modulation[s, l] for l in range(LAYERS)] + [None] for s in range(seqs)]
    ready = [low([step.start(rows[s], mods[s][0])])[0] for s in range(seqs)]
    last = LAYERS - 1
    db2 = [low([step.pick(mods[s][last], 5) * upstream[s]])[0] for s in range(seqs)]
    for l in range(LAYERS):
        done = [step.forward(rows[s], ready[s], mods[s][l], mods[s][l + 1], weights[l], masks[s]) for s in range(seqs)]
        rows, ready = [d[0] for d in done], [d[1] for d in done]
        saved.append([d[2] for d in done])
    image_output, text_output = undeal(rows)

    reduced, mod_rows = [None] * LAYERS, [None] * LAYERS
    for l in reversed(range(LAYERS)):
        mlp = [step.backward_mlp(upstream[s], db2[s], saved[l][s], weights[l]) for s in range(seqs)]
        down_total = weight_grads([m[4] for m in mlp])
        up_total = weight_grads([m[3] for m in mlp])
        db1 = [m[2] for m in mlp]
        grad_down = reduce_weight(down_total)
        grad_up = reduce_weight(up_total)
        if l < last:
            db1[0], reduced[l + 1] = tie(db1[0], reduced[l + 1])
        att = [
            step.backward_attention(mlp[s][0], db1[s], saved[l][s], mods[s][l - 1] if l else None, weights[l], masks[s])
            for s in range(seqs)
        ]
        out_total = weight_grads([a[4] for a in att])
        qkv_total = weight_grads([a[3] for a in att])
        upstream, db2 = [a[0] for a in att], [a[1] for a in att]
        if l:
            db2[1], out_total, qkv_total = tie(db2[1], out_total, qkv_total)
        grad_out = reduce_weight(out_total)
        grad_qkv = reduce_weight(qkv_total)
        mod_rows[l] = jnp.stack([jnp.concatenate([att[s][2], mlp[s][1]], axis=1) for s in range(seqs)])
        reduced[l] = [grad_qkv, grad_out, grad_up, grad_down]
    image_grad, text_grad = undeal(upstream)
    reduced = [[r.astype(F32) for r in layer] for layer in reduced]

    mod_rows = jnp.stack(mod_rows, axis=1).reshape(-1, mp_size, columns)
    mod_sums = exchange_sum(jnp.swapaxes(mod_rows, 0, 1).reshape(mp_size, -1, columns), "mp")
    all_mods = lax.all_gather(mod_sums, "dp", axis=0).reshape(-1, LAYERS, 2, 6, columns)
    grad_mod = jnp.einsum("nd,nlskc->lsdkc", own_condition.astype(F32), all_mods, precision=lax.Precision.HIGHEST)
    grad_qkv = jnp.stack(
        [jnp.swapaxes(r[0].reshape(2, -1, 3, columns), 1, 2) for r in reduced]
    )
    return (
        image_output,
        text_output,
        image_grad,
        text_grad,
        grad_mod,
        grad_qkv,
        jnp.stack([jnp.swapaxes(r[1], 1, 2) for r in reduced]),
        jnp.stack([r[2] for r in reduced]),
        jnp.stack([jnp.swapaxes(r[3], 1, 2) for r in reduced]),
    )


def solution(mesh):
    rows = P(("dp", "mp"), None)
    grads = (
        P(None, None, "dp", None, "mp"),
        P(None, None, None, "dp", "mp"),
        P(None, None, "mp", "dp"),
        P(None, None, "dp", "mp"),
        P(None, None, "mp", "dp"),
    )

    def program(*arrays):
        return device_program(mesh.shape["mp"], *arrays)

    return jax.shard_map(
        program,
        mesh=mesh,
        in_specs=(rows, rows, P(), P("dp", None)) + grads + (rows, rows),
        out_specs=(rows, rows, rows, rows) + grads,
        check_vma=False,
    )
```
